32 devices in a mesh: seq: 8 (over z, core), head: 4 (over y, x).
Axes of the slice: x: 2, y: 2, z: 4, core: 2. Of those that a mesh axis runs over, the one named last changes fastest.
Arguments:
- inputs: float32 [2048, 2048], P('seq', 'head'), may hold values from -6 to 6
- w_project: float32 [2048, 3, 2048], P('seq', None, 'head'), may hold values from -0.125 to 0.125
- w_output: float32 [2048, 2048], P('head', 'seq'), may hold values from -0.1875 to 0.1875
- norm_gain: float32 [2048], P('head'), may hold values from 0.1 to 1.9
Outputs:
- mixed: float32 [2048, 2048], P('seq', 'head')
The draws below stay inside these ranges and needn't reach their ends.
All inputs are finite; a program needn't handle non-finite values.
Results may differ from the reference program's by a relative error of at most 0.0003.
Values sent between devices are 32-bit elements; how exact they have to be, the bound alone decides.
No kernel may reach another device: no remote copies, remote signals or barrier semaphores. Data moves between devices by JAX's collectives and lax.ppermute only.
A program may use at most 64 MiB of HBM per device.

```python
import jax
import jax.numpy as jnp
from jax import lax

D = 2048
HEADS = 16
DK = 128
SPAN = 64
TOKENS = 2048


def strengthened(values, rng, source, target, parts, factor):
    def block_of(axis_at):
        return (jnp.arange(values.shape[axis_at]) // (values.shape[axis_at] // parts)).reshape((-1,) + (1,) * (values.ndim - 1 - axis_at))

    one_side = jax.random.permutation(rng, parts)[block_of(target)]
    second = (block_of(target) + parts // 2) % parts
    return jnp.where((block_of(source) == one_side) | (block_of(source) == second), factor * values, values)


def level_of(own_key, extent, cuts, low, largest):
    level = 1.0
    for position, parts in cuts:
        steps = jax.random.uniform(jax.random.fold_in(jax.random.fold_in(own_key, 6), position), (parts,), jnp.float32, low / len(cuts), largest / len(cuts))
        level = level * jnp.repeat(jnp.exp(steps), extent[position] // parts).reshape((-1,) + (1,) * (len(extent) - 1 - position))
    return level


def bell_draw(rng, shape, spread, most, pieces=(), held_as=jnp.bfloat16):
    entries = jax.random.normal(rng, shape, jnp.float32) * spread
    if len(pieces) > 0:
        entries = level_of(rng, shape, pieces, -0.22, 0.18) * entries
    return jnp.clip(entries, min=-most, max=most).astype(held_as)


def heavy_noise(stream_key, extent, scale, most, cuts, heavy, held_as=jnp.bfloat16):
    array = scale * jax.random.normal(stream_key, extent, jnp.float32)
    if cuts:
        array = array * level_of(stream_key, extent, cuts, -0.22, 0.18)
    return jnp.clip(strengthened(array, jax.random.fold_in(stream_key, 3), *heavy), -most, most).astype(held_as)


def setup_inputs(seed: int = 0) -> dict:
    arg_keys = jax.random.split(jax.random.key(seed), 5)
    inputs = bell_draw(arg_keys[0], (TOKENS, D), 1.0, 6.0, ((0, 8), (1, 4)), jnp.float32)
    w_project = bell_draw(arg_keys[1], (D, 3, HEADS * DK), D ** -0.5, 0.125, ((0, 8), (2, 4)), jnp.float32)
    w_output = heavy_noise(arg_keys[2], (HEADS * DK, D), (HEADS * DK) ** -0.5, 0.1875, ((0, 4), (1, 8)), (0, 1, 8, 2.0), jnp.float32)
    norm_gain = jnp.clip(1.0 + 0.18 * jax.random.normal(arg_keys[3], (HEADS * DK,), jnp.float32), 0.1, 1.9)
    return dict(inputs=inputs, w_project=w_project, w_output=w_output, norm_gain=norm_gain)


HIGH = lax.Precision.HIGHEST

def unit_rows(matrix):
    return matrix * lax.rsqrt(lax.optimization_barrier(jnp.sum(matrix * matrix, axis=-1, keepdims=True)) + 1e-06)

def block_terms(queries, keys, values):
    width = keys.shape[-1]
    length = keys.shape[-2]
    inner = jnp.einsum('...ck,...dk->...cd', keys, keys, precision=HIGH)
    strict = jnp.tril(jnp.ones((length, length), jnp.float32), -1)
    system = jnp.eye(length, dtype=jnp.float32) + 2.0 * strict * inner
    system = jnp.broadcast_to(system, inner.shape)
    stacked = 2.0 * jnp.concatenate([keys, values], axis=-1)
    solved = lax.linalg.triangular_solve(system, stacked, left_side=True, lower=True, unit_diagonal=True)
    w_rows = solved[..., :width]
    u_rows = solved[..., width:]
    transit = jnp.eye(width, dtype=jnp.float32) - jnp.einsum('...cw,...ck->...wk', w_rows, keys, precision=HIGH)
    written = jnp.einsum('...cv,...ck->...vk', u_rows, keys, precision=HIGH)
    causal = jnp.tril(jnp.einsum('...ck,...dk->...cd', queries, keys, precision=HIGH))
    local_out = jnp.einsum('...cd,...dv->...cv', causal, u_rows, precision=HIGH)
    reach = queries - jnp.einsum('...cd,...dk->...ck', causal, w_rows, precision=HIGH)
    return (transit, written, local_out, reach)

def reference(inputs, w_project, w_output, norm_gain):
    proj = jnp.dot(inputs.astype(jnp.float32), w_project.reshape(D, 3 * HEADS * DK).astype(jnp.float32), precision=HIGH, preferred_element_type=jnp.float32)
    proj = jnp.transpose(proj.reshape(TOKENS // SPAN, SPAN, 3, HEADS, DK), (2, 0, 3, 1, 4))
    queries = unit_rows(proj[0])
    keys = unit_rows(proj[1])
    values = proj[2]

    def advance(state, block):
        transit, written, local_out, reach = block_terms(block[0], block[1], block[2])
        result = local_out + jnp.einsum('hck,hvk->hcv', reach, state, precision=HIGH)
        following = jnp.einsum('hvk,hkj->hvj', state, transit, precision=HIGH) + written
        return (following, result)
    start = jnp.zeros((HEADS, DK, DK), jnp.float32)
    _, outputs = lax.scan(advance, start, (queries, keys, values))
    outputs = jnp.transpose(outputs, (0, 2, 1, 3)).reshape(TOKENS, HEADS, DK)
    normed = outputs * lax.rsqrt(lax.optimization_barrier(jnp.mean(outputs * outputs, axis=-1, keepdims=True)) + 1e-06)
    normed = normed.reshape(TOKENS, HEADS * DK) * norm_gain
    return jnp.dot(normed.astype(jnp.float32), w_output.astype(jnp.float32), precision=HIGH, preferred_element_type=jnp.float32)
```

```python
import functools

import jax
import jax.numpy as jnp
from jax import lax
from jax.experimental import pallas as pl
from jax.experimental.pallas import tpu as pltpu
from jax.sharding import PartitionSpec as P

DK = 128
SPAN = 64
BLOCK = 256


HIGH = lax.Precision.HIGHEST
THREE = lax.Precision.HIGH


def from_behind(shard, axis, by):
    size = lax.axis_size(axis)
    pairs = [(i, i + by) for i in range(size) if 0 <= i + by < size]
    return lax.ppermute(shard, axis, pairs)


def unit_rows(matrix):
    return matrix * lax.rsqrt(jnp.sum(matrix * matrix, axis=-1, keepdims=True) + 1e-06)


def block_terms(queries, keys, values):
    width = keys.shape[-1]
    length = keys.shape[-2]
    inner = jnp.einsum("...ck,...dk->...cd", keys, keys, precision=HIGH)
    strict = jnp.tril(jnp.ones((length, length), jnp.float32), -1)
    system = jnp.eye(length, dtype=jnp.float32) + 2.0 * strict * inner
    stacked = 2.0 * jnp.concatenate([keys, values], axis=-1)
    solved = lax.linalg.triangular_solve(
        system, stacked, left_side=True, lower=True, unit_diagonal=True
    )
    w_rows = solved[..., :width]
    u_rows = solved[..., width:]
    transit = jnp.eye(width, dtype=jnp.float32) - jnp.einsum(
        "...cw,...ck->...wk", w_rows, keys, precision=HIGH
    )
    written = jnp.einsum("...cv,...ck->...vk", u_rows, keys, precision=HIGH)
    causal = jnp.tril(jnp.einsum("...ck,...dk->...cd", queries, keys, precision=HIGH))
    local_out = jnp.einsum("...cd,...dv->...cv", causal, u_rows, precision=HIGH)
    reach = queries - jnp.einsum("...cd,...dk->...ck", causal, w_rows, precision=HIGH)
    return (transit, written, local_out, reach)


def compose(first, second):
    return jnp.einsum("hvk,hkj->hvj", first, second, precision=HIGH)


def general(inputs, w_project, w_output, norm_gain):
    tok_rows = inputs.shape[0]
    columns = w_project.shape[2]
    heads = columns // DK
    blocks = tok_rows // SPAN
    features = lax.all_gather(inputs, "head", axis=1, tiled=True)
    proj = jnp.einsum(
        "td,dgc->tgc",
        features,
        lax.all_gather(w_project, "seq", axis=0, tiled=True),
        precision=HIGH,
    )
    proj = jnp.transpose(proj.reshape(blocks, SPAN, 3, heads, DK), (2, 0, 3, 1, 4))
    queries = unit_rows(proj[0])
    keys = unit_rows(proj[1])
    values = proj[2]
    transit, written, local_out, reach = block_terms(queries, keys, values)
    identity = jnp.broadcast_to(jnp.eye(DK, dtype=jnp.float32), (heads, DK, DK))
    nothing = jnp.zeros((heads, DK, DK), jnp.float32)

    def chain(carry, pair):
        acc_transit, acc_written = carry
        following = (compose(acc_transit, pair[0]), compose(acc_written, pair[0]) + pair[1])
        return (following, carry)

    (dev_transit, dev_written), (before_transit, before_written) = lax.scan(
        chain, (identity, nothing), (transit, written)
    )

    def relay_turn(turn, incoming):
        leaving = compose(incoming, dev_transit) + dev_written
        return from_behind(leaving, "seq", 1)

    entry = lax.fori_loop(0, lax.axis_size("seq") - 1, relay_turn, nothing)
    starts = jnp.einsum("hvk,nhkj->nhvj", entry, before_transit, precision=HIGH) + before_written
    outputs = local_out + jnp.einsum("nhck,nhvk->nhcv", reach, starts, precision=HIGH)
    outputs = jnp.transpose(outputs, (0, 2, 1, 3)).reshape(tok_rows, heads, DK)
    normed = outputs * lax.rsqrt(jnp.mean(outputs * outputs, axis=-1, keepdims=True) + 1e-06)
    normed = normed.reshape(tok_rows, heads * DK) * norm_gain
    partial_sums = jnp.dot(
        normed,
        lax.all_gather(w_output, "seq", axis=1, tiled=True),
        precision=HIGH,
        preferred_element_type=jnp.float32,
    )
    return lax.psum_scatter(partial_sums, "head", scatter_dimension=1, tiled=True)


def halves(a):
    top = a.astype(jnp.bfloat16)
    return top, (a - top.astype(jnp.float32)).astype(jnp.bfloat16)


def mul3(a, b, dims=((1,), (0,))):
    dot = functools.partial(
        lax.dot_general, dimension_numbers=(dims, ((), ())), preferred_element_type=jnp.float32
    )
    return dot(a[0], b[0]) + (dot(a[0], b[1]) + dot(a[1], b[0]))


def dot3(a, b, dims=((1,), (0,))):
    return mul3(halves(a), halves(b), dims)


def terms_kernel(k_ref, v_ref, keys_ref, w_ref, u_ref, end_ref, low_ref, inv_ref):
    groups = low_ref.shape[0]
    row = lax.broadcasted_iota(jnp.int32, (BLOCK, BLOCK), 0)
    col = lax.broadcasted_iota(jnp.int32, (BLOCK, BLOCK), 1)
    for n in range(groups):
        part = pl.ds(n * BLOCK, BLOCK)
        raw = k_ref[part, :]
        keys = raw * lax.rsqrt(jnp.sum(raw * raw, axis=-1, keepdims=True) + 1e-06)
        keys_ref[part, :] = keys
        pair = halves(keys)
        low = jnp.where(row > col, 2.0 * mul3(pair, pair, ((1,), (1,))), 0.0)
        low_ref[n] = low
        inv_ref[n] = jnp.where(row == col, 1.0, jnp.where((row >> 1) == (col >> 1), -low, 0.0))

    def level(at, carry):
        here = ((row >> (at + 1)) == (col >> (at + 1))) & ((row >> at) != (col >> at))
        for n in range(groups):
            inverse = inv_ref[n]
            pair = halves(inverse)
            off = jnp.where(here, low_ref[n], 0.0)
            inv_ref[n] = inverse - mul3(pair, halves(mul3(halves(off), pair)))
        return carry

    lax.fori_loop(1, BLOCK.bit_length() - 1, level, 0)
    for n in range(groups):
        part = pl.ds(n * BLOCK, BLOCK)
        inverse = halves(inv_ref[n])
        w_ref[part, :] = mul3(inverse, halves(2.0 * keys_ref[part, :]))
        u_ref[part, :] = mul3(inverse, halves(2.0 * v_ref[part, :]))
    state = jnp.zeros((DK, DK), jnp.float32)
    for n in range(groups):
        part = pl.ds(n * BLOCK, BLOCK)
        fresh = u_ref[part, :]
        if n > 0:
            fresh = fresh - dot3(w_ref[part, :], state)
        state = state + dot3(keys_ref[part, :], fresh, ((0,), (0,)))
    end_ref[...] = state


def leave_kernel(start_ref, keys_ref, w_ref, u_ref, end_ref):
    state = start_ref[...]
    for n in range(keys_ref.shape[0] // BLOCK):
        part = pl.ds(n * BLOCK, BLOCK)
        fresh = u_ref[part, :] - dot3(w_ref[part, :], state)
        state = state + dot3(keys_ref[part, :], fresh, ((0,), (0,)))
    end_ref[...] = state


def output_kernel(start_ref, q_ref, keys_ref, w_ref, u_ref, gain_ref, out_ref):
    row = lax.broadcasted_iota(jnp.int32, (BLOCK, BLOCK), 0)
    col = lax.broadcasted_iota(jnp.int32, (BLOCK, BLOCK), 1)
    state = start_ref[...]
    for n in range(keys_ref.shape[0] // BLOCK):
        part = pl.ds(n * BLOCK, BLOCK)
        raw = q_ref[part, :]
        queries = halves(raw * lax.rsqrt(jnp.sum(raw * raw, axis=-1, keepdims=True) + 1e-06))
        keys = halves(keys_ref[part, :])
        causal = jnp.where(row >= col, mul3(queries, keys, ((1,), (1,))), 0.0)
        entry = halves(state)
        fresh = halves(u_ref[part, :] - mul3(halves(w_ref[part, :]), entry))
        result = mul3(queries, entry) + mul3(halves(causal), fresh)
        state = state + mul3(keys, fresh, ((0,), (0,)))
        scale = lax.rsqrt(jnp.mean(result * result, axis=-1, keepdims=True) + 1e-06)
        out_ref[part, :] = result * scale * gain_ref[...]


def f32(*shape):
    return jax.ShapeDtypeStruct(shape, jnp.float32)


def chain_terms(k, v):
    rows = k.shape[0]
    groups = rows // BLOCK
    flops = 3 * 2 * groups * BLOCK * BLOCK * BLOCK * 17
    return pl.pallas_call(
        terms_kernel,
        out_shape=(f32(rows, DK), f32(rows, DK), f32(rows, DK), f32(DK, DK)),
        scratch_shapes=[pltpu.VMEM((groups, BLOCK, BLOCK), jnp.float32)] * 2,
        cost_estimate=pl.CostEstimate(flops=flops, bytes_accessed=20 * rows * DK, transcendentals=rows),
        name="chain_terms",
    )(k, v)


def chain_leave(start, keys, w, u):
    rows = keys.shape[0]
    return pl.pallas_call(
        leave_kernel,
        out_shape=f32(DK, DK),
        cost_estimate=pl.CostEstimate(
            flops=3 * 4 * rows * DK * DK, bytes_accessed=12 * rows * DK, transcendentals=0
        ),
        name="chain_leave",
    )(start, keys, w, u)


def chain_output(start, q, keys, w, u, gain):
    rows = keys.shape[0]
    return pl.pallas_call(
        output_kernel,
        out_shape=f32(rows, DK),
        cost_estimate=pl.CostEstimate(
            flops=3 * 2 * rows * DK * (3 * DK + 2 * BLOCK), bytes_accessed=20 * rows * DK, transcendentals=2 * rows
        ),
        name="chain_output",
    )(start, q, keys, w, u, gain)


def by_xor(shard, axis, with_):
    size = lax.axis_size(axis)
    return lax.ppermute(shard, axis, [(i, i ^ with_) for i in range(size)])


def place(whole, piece, at):
    return lax.dynamic_update_slice_in_dim(whole, piece, at, 0)


def exchanged(inputs, w_project, w_output, norm_gain):
    rows, feats = inputs.shape
    heads = w_project.shape[2] // DK
    seq = lax.axis_size("seq")
    groups = lax.axis_size("head")
    spans = seq // heads
    s = lax.axis_index("seq")
    h = lax.axis_index("head")
    j = s % heads
    w_rows = w_project.shape[0]
    own = w_project.reshape(w_rows, 3, heads, DK).transpose(2, 0, 1, 3).reshape(heads, w_rows, 3 * DK)
    sent = jnp.broadcast_to(own[None], (spans, heads, w_rows, 3 * DK)).reshape(seq, w_rows, 3 * DK)
    weights = lax.all_to_all(sent, "seq", split_axis=0, concat_axis=0, tiled=True)
    weights = weights.reshape(seq * w_rows, 3 * DK)

    def all_features(block):
        pieces = [(block, h)] + [(by_xor(block, "head", g), h ^ g) for g in range(1, groups)]
        whole = jnp.zeros((rows, groups * feats), jnp.float32)
        for piece, at in pieces:
            whole = lax.dynamic_update_slice_in_dim(whole, piece, at * feats, 1)
        return whole

    token_parts = {}
    for far in range(0, heads, 2):
        block = inputs if far == 0 else by_xor(inputs, "seq", far)
        token_parts[far] = all_features(block)
    for far in range(0, heads, 2):
        token_parts[far + 1] = by_xor(token_parts[far], "seq", 1)
    proj = jnp.zeros((heads * rows, 3 * DK), jnp.float32)
    for far in range(heads):
        proj = place(proj, jnp.dot(token_parts[far], weights, precision=THREE), (j ^ far) * rows)

    pairs = seq // 2
    mine = w_output[None]
    right, left = mine, mine
    rights, lefts = [], []
    for _ in range(pairs - 1):
        right = lax.ppermute(right, "seq", [(i, i + 2) for i in range(seq - 2)])
        left = lax.ppermute(left, "seq", [(i + 2, i) for i in range(seq - 2)])
        rights.append(right)
        lefts.append(left)
    line = jnp.concatenate(rights[::-1] + [mine] + lefts, axis=0)
    w_out_mine = lax.dynamic_slice_in_dim(line, pairs - 1 - s // 2, pairs, 0)
    w_out_sibling = by_xor(w_out_mine, "seq", 1)

    q, k, v = proj[:, :DK], proj[:, DK : 2 * DK], proj[:, 2 * DK :]
    keys, w, u, leaving = chain_terms(k, v)
    start = jnp.zeros((DK, DK), jnp.float32)
    for turn in range(spans - 1):
        if turn > 0:
            leaving = chain_leave(start, keys, w, u)
        start = from_behind(leaving, "seq", heads)
    gain = lax.dynamic_slice_in_dim(norm_gain, j * DK, DK, 0).reshape(1, DK)
    normed = chain_output(start, q, keys, w, u, gain)

    def tokens_of(at):
        return lax.dynamic_slice_in_dim(normed, at * rows, rows, 0)

    back = jnp.zeros((rows, heads * DK), jnp.float32)
    for far in range(heads):
        piece = tokens_of(j ^ far)
        if far:
            piece = by_xor(piece, "seq", far)
        back = lax.dynamic_update_slice_in_dim(back, piece, (j ^ far) * DK, 1)

    part_mine = jnp.einsum("tf,pfc->ptc", back, w_out_mine, precision=THREE)
    part_sibling = jnp.einsum("tf,pfc->ptc", back, w_out_sibling, precision=THREE)
    odd = s % 2 == 1
    first = jnp.where(odd, part_sibling, part_mine)
    second = jnp.where(odd, part_mine, part_sibling)
    part = jnp.concatenate([first, second], axis=-1)
    per = pairs // groups
    part = part.reshape(groups, per, rows, -1).transpose(0, 2, 1, 3).reshape(groups, rows, -1)
    total = lax.dynamic_index_in_dim(part, h, 0, keepdims=False)
    for g in range(1, groups):
        total = total + by_xor(lax.dynamic_index_in_dim(part, h ^ g, 0, keepdims=False), "head", g)
    return total


def power_of_two(n):
    return n > 0 and n & (n - 1) == 0


def solution(mesh):
    seq, groups = mesh.shape["seq"], mesh.shape["head"]

    def step(inputs, w_project, w_output, norm_gain):
        heads = w_project.shape[2] // DK
        fits = (
            power_of_two(seq)
            and power_of_two(groups)
            and power_of_two(heads)
            and 2 <= heads <= seq
            and (seq // 2) % groups == 0
            and inputs.shape[0] * heads % BLOCK == 0
        )
        plan = exchanged if fits else general
        return plan(inputs, w_project, w_output, norm_gain)

    return jax.shard_map(
        step,
        mesh=mesh,
        in_specs=(P("seq", "head"), P("seq", None, "head"), P("head", "seq"), P("head")),
        out_specs=P("seq", "head"),
        check_vma=False,
    )
```

```python
import functools

import jax
import jax.numpy as jnp
from jax import lax
from jax.experimental import pallas as pl
from jax.experimental.pallas import tpu as pltpu
from jax.sharding import PartitionSpec as P


DK = 128
SPAN = 64
BLOCK = 256


HIGH = lax.Precision.HIGHEST


def from_behind(shard, axis, by):
    size = lax.axis_size(axis)
    pairs = [(i, i + by) for i in range(size) if 0 <= i + by < size]
    return lax.ppermute(shard, axis, pairs)


def unit_rows(matrix):
    return matrix * lax.rsqrt(jnp.sum(matrix * matrix, axis=-1, keepdims=True) + 1e-06)


def block_terms(queries, keys, values):
    width = keys.shape[-1]
    length = keys.shape[-2]
    inner = jnp.einsum("...ck,...dk->...cd", keys, keys, precision=HIGH)
    strict = jnp.tril(jnp.ones((length, length), jnp.float32), -1)
    system = jnp.eye(length, dtype=jnp.float32) + 2.0 * strict * inner
    stacked = 2.0 * jnp.concatenate([keys, values], axis=-1)
    solved = lax.linalg.triangular_solve(
        system, stacked, left_side=True, lower=True, unit_diagonal=True
    )
    w_rows = solved[..., :width]
    u_rows = solved[..., width:]
    transit = jnp.eye(width, dtype=jnp.float32) - jnp.einsum(
        "...cw,...ck->...wk", w_rows, keys, precision=HIGH
    )
    written = jnp.einsum("...cv,...ck->...vk", u_rows, keys, precision=HIGH)
    causal = jnp.tril(jnp.einsum("...ck,...dk->...cd", queries, keys, precision=HIGH))
    local_out = jnp.einsum("...cd,...dv->...cv", causal, u_rows, precision=HIGH)
    reach = queries - jnp.einsum("...cd,...dk->...ck", causal, w_rows, precision=HIGH)
    return (transit, written, local_out, reach)


def compose(first, second):
    return jnp.einsum("hvk,hkj->hvj", first, second, precision=HIGH)


def general(inputs, w_project, w_output, norm_gain):
    tok_rows = inputs.shape[0]
    columns = w_project.shape[2]
    heads = columns // DK
    blocks = tok_rows // SPAN
    features = lax.all_gather(inputs, "head", axis=1, tiled=True)
    proj = jnp.einsum(
        "td,dgc->tgc",
        features,
        lax.all_gather(w_project, "seq", axis=0, tiled=True),
        precision=HIGH,
    )
    proj = jnp.transpose(proj.reshape(blocks, SPAN, 3, heads, DK), (2, 0, 3, 1, 4))
    queries = unit_rows(proj[0])
    keys = unit_rows(proj[1])
    values = proj[2]
    transit, written, local_out, reach = block_terms(queries, keys, values)
    identity = jnp.broadcast_to(jnp.eye(DK, dtype=jnp.float32), (heads, DK, DK))
    nothing = jnp.zeros((heads, DK, DK), jnp.float32)

    def chain(carry, pair):
        acc_transit, acc_written = carry
        following = (compose(acc_transit, pair[0]), compose(acc_written, pair[0]) + pair[1])
        return (following, carry)

    (dev_transit, dev_written), (before_transit, before_written) = lax.scan(
        chain, (identity, nothing), (transit, written)
    )

    def relay_turn(turn, incoming):
        leaving = compose(incoming, dev_transit) + dev_written
        return from_behind(leaving, "seq", 1)

    entry = lax.fori_loop(0, lax.axis_size("seq") - 1, relay_turn, nothing)
    starts = jnp.einsum("hvk,nhkj->nhvj", entry, before_transit, precision=HIGH) + before_written
    outputs = local_out + jnp.einsum("nhck,nhvk->nhcv", reach, starts, precision=HIGH)
    outputs = jnp.transpose(outputs, (0, 2, 1, 3)).reshape(tok_rows, heads, DK)
    normed = outputs * lax.rsqrt(jnp.mean(outputs * outputs, axis=-1, keepdims=True) + 1e-06)
    normed = normed.reshape(tok_rows, heads * DK) * norm_gain
    partial_sums = jnp.dot(
        normed,
        lax.all_gather(w_output, "seq", axis=1, tiled=True),
        precision=HIGH,
        preferred_element_type=jnp.float32,
    )
    return lax.psum_scatter(partial_sums, "head", scatter_dimension=1, tiled=True)


def halves(a):
    top = a.astype(jnp.bfloat16)
    return top, (a - top.astype(jnp.float32)).astype(jnp.bfloat16)


def mul3(a, b, dims=((1,), (0,))):
    dot = functools.partial(
        lax.dot_general, dimension_numbers=(dims, ((), ())), preferred_element_type=jnp.float32
    )
    return dot(a[0], b[0]) + (dot(a[0], b[1]) + dot(a[1], b[0]))


def dot3(a, b, dims=((1,), (0,))):
    return mul3(halves(a), halves(b), dims)


def terms_kernel(k_ref, v_ref, keys_ref, w_ref, u_ref, end_ref, low_ref, inv_ref):
    groups = low_ref.shape[0]
    row = lax.broadcasted_iota(jnp.int32, (BLOCK, BLOCK), 0)
    col = lax.broadcasted_iota(jnp.int32, (BLOCK, BLOCK), 1)
    for n in range(groups):
        part = pl.ds(n * BLOCK, BLOCK)
        raw = k_ref[part, :]
        keys = raw * lax.rsqrt(jnp.sum(raw * raw, axis=-1, keepdims=True) + 1e-06)
        keys_ref[part, :] = keys
        pair = halves(keys)
        low = jnp.where(row > col, 2.0 * mul3(pair, pair, ((1,), (1,))), 0.0)
        low_ref[n] = low
        inv_ref[n] = jnp.where(row == col, 1.0, jnp.where((row >> 1) == (col >> 1), -low, 0.0))

    def level(at, carry):
        here = ((row >> (at + 1)) == (col >> (at + 1))) & ((row >> at) != (col >> at))
        for n in range(groups):
            inverse = inv_ref[n]
            pair = halves(inverse)
            off = jnp.where(here, low_ref[n], 0.0)
            inv_ref[n] = inverse - mul3(pair, halves(mul3(halves(off), pair)))
        return carry

    lax.fori_loop(1, BLOCK.bit_length() - 1, level, 0)
    for n in range(groups):
        part = pl.ds(n * BLOCK, BLOCK)
        inverse = halves(inv_ref[n])
        w_ref[part, :] = mul3(inverse, halves(2.0 * keys_ref[part, :]))
        u_ref[part, :] = mul3(inverse, halves(2.0 * v_ref[part, :]))
    state = jnp.zeros((DK, DK), jnp.float32)
    for n in range(groups):
        part = pl.ds(n * BLOCK, BLOCK)
        fresh = u_ref[part, :]
        if n > 0:
            fresh = fresh - dot3(w_ref[part, :], state)
        state = state + dot3(keys_ref[part, :], fresh, ((0,), (0,)))
    end_ref[...] = state


def leave_kernel(start_ref, keys_ref, w_ref, u_ref, end_ref):
    state = start_ref[...]
    for n in range(keys_ref.shape[0] // BLOCK):
        part = pl.ds(n * BLOCK, BLOCK)
        fresh = u_ref[part, :] - dot3(w_ref[part, :], state)
        state = state + dot3(keys_ref[part, :], fresh, ((0,), (0,)))
    end_ref[...] = state


def output_kernel(at_ref, start_ref, q_ref, keys_ref, w_ref, u_ref, gain_ref, *outs):
    heads = len(outs)
    j = at_ref[0] % heads
    gain = gain_ref[j]
    row = lax.broadcasted_iota(jnp.int32, (BLOCK, BLOCK), 0)
    col = lax.broadcasted_iota(jnp.int32, (BLOCK, BLOCK), 1)
    state = start_ref[...]
    for n in range(keys_ref.shape[0] // BLOCK):
        part = pl.ds(n * BLOCK, BLOCK)
        raw = q_ref[part, :]
        queries = halves(raw * lax.rsqrt(jnp.sum(raw * raw, axis=-1, keepdims=True) + 1e-06))
        keys = halves(keys_ref[part, :])
        causal = jnp.where(row >= col, mul3(queries, keys, ((1,), (1,))), 0.0)
        entry = halves(state)
        fresh = halves(u_ref[part, :] - mul3(halves(w_ref[part, :]), entry))
        result = mul3(queries, entry) + mul3(halves(causal), fresh)
        state = state + mul3(keys, fresh, ((0,), (0,)))
        result = result * lax.rsqrt(jnp.mean(result * result, axis=-1, keepdims=True) + 1e-06) * gain
        for far in range(heads):

            @pl.when((j ^ far) == n)
            def _():
                outs[far][...] = result


def f32(*shape):
    return jax.ShapeDtypeStruct(shape, jnp.float32)


def column(rows, at):
    return pl.BlockSpec((rows, DK), lambda i: (0, at))


def chain_terms(proj):
    rows = proj.shape[0]
    groups = rows // BLOCK
    flops = 3 * 2 * groups * BLOCK * BLOCK * BLOCK * 17
    return pl.pallas_call(
        terms_kernel,
        grid=(1,),
        in_specs=[column(rows, 1), column(rows, 2)],
        out_specs=[column(rows, 0)] * 3 + [column(DK, 0)],
        out_shape=(f32(rows, DK), f32(rows, DK), f32(rows, DK), f32(DK, DK)),
        scratch_shapes=[pltpu.VMEM((groups, BLOCK, BLOCK), jnp.float32)] * 2,
        cost_estimate=pl.CostEstimate(flops=flops, bytes_accessed=20 * rows * DK, transcendentals=rows),
        name="chain_terms",
    )(proj, proj)


def chain_leave(start, keys, w, u):
    rows = keys.shape[0]
    return pl.pallas_call(
        leave_kernel,
        out_shape=f32(DK, DK),
        cost_estimate=pl.CostEstimate(
            flops=3 * 4 * rows * DK * DK, bytes_accessed=12 * rows * DK, transcendentals=0
        ),
        name="chain_leave",
    )(start, keys, w, u)


def chain_output(start, proj, keys, w, u, gain, at, token_rows):
    rows = keys.shape[0]
    heads = rows // token_rows
    return pl.pallas_call(
        output_kernel,
        grid=(1,),
        in_specs=[SCALARS, column(DK, 0), column(rows, 0)]
        + [column(rows, 0)] * 3
        + [pl.BlockSpec((heads, 1, DK), lambda i: (0, 0, 0))],
        out_specs=[column(token_rows, 0)] * heads,
        out_shape=[f32(token_rows, DK)] * heads,
        cost_estimate=pl.CostEstimate(
            flops=3 * 2 * rows * DK * (3 * DK + 2 * BLOCK), bytes_accessed=20 * rows * DK, transcendentals=2 * rows
        ),
        name="chain_output",
    )(at, start, proj, keys, w, u, gain)


def on_chip(n):
    return [pl.BlockSpec(memory_space=pltpu.VMEM)] * n


SCALARS = pl.BlockSpec(memory_space=pltpu.SMEM)


def columns_kernel(at_ref, w_ref, *outs):
    heads = len(outs)
    mine = at_ref[0] % heads
    for near in range(heads):
        for slot in range(heads):

            @pl.when((mine ^ near) == slot)
            def _():
                for part in range(w_ref.shape[0]):
                    outs[near][:, part * DK : (part + 1) * DK] = w_ref[part, :, slot * DK : (slot + 1) * DK]


def head_columns(at, w):
    parts, rows, width = w.shape
    return pl.pallas_call(
        columns_kernel,
        in_specs=[SCALARS] + on_chip(1),
        out_shape=[f32(rows, parts * DK)] * (width // DK),
        name="head_columns",
    )(at, w)


def project_kernel(heads, span, at_ref, *refs):
    tokens = refs[: 2 * GROUPS]
    weights = refs[2 * GROUPS : 2 * GROUPS + heads]
    before = refs[2 * GROUPS + heads : -5]
    out_ref, x_ref, top_ref, rem_ref, sem = refs[-5:]
    s, h = at_ref[0], at_ref[1]
    j, m = s % heads, (s // heads) ^ span
    upper = (h >> 1) ^ m
    rows = out_ref.shape[0] // 4

    def loads(half, go):
        for side in range(2):
            for t in range(2):
                copy = pltpu.make_async_copy(tokens[side * GROUPS + 2 * half + t], x_ref.at[side, t], sem.at[side, t])
                copy.start() if go else copy.wait()

    for half in range(2):

        @pl.when(upper == half)
        def _():
            loads(half, True)

    w_rows = weights[0].shape[0]
    for near in range(heads):
        r = j ^ near
        spot = pl.multiple_of((r ^ ((h & 1) << 1)) * w_rows, w_rows)
        top_ref[pl.ds(spot, w_rows), :], rem_ref[pl.ds(spot, w_rows), :] = halves(weights[near][...])
    dot = functools.partial(jnp.dot, preferred_element_type=jnp.float32)
    feats = x_ref.shape[-1]
    for side in range(2):
        for t in range(2):
            pltpu.make_async_copy(tokens[side * GROUPS], x_ref.at[side, t], sem.at[side, t]).wait()
            part = pl.ds(t * feats, feats)
            w_top, w_rem = top_ref[part, :], rem_ref[part, :]
            for b in range(2):
                top, rem = halves(x_ref[side, t, b * rows : (b + 1) * rows, :])
                to = pl.ds(pl.multiple_of((j ^ (side + 2 * b)) * rows, rows), rows)
                total = dot(top, w_top) + (dot(top, w_rem) + dot(rem, w_top))
                if t == 1:
                    total = total + out_ref[to, :]
                elif before:
                    total = total + before[0][to, :]
                out_ref[to, :] = total


GROUPS = 4


def project(at, tokens, weights, span, before=None):
    heads = len(weights)
    side_rows, feats = tokens[0].shape
    width = weights[0].shape[1]
    extra = () if before is None else (before,)
    return pl.pallas_call(
        functools.partial(project_kernel, heads, span),
        in_specs=[SCALARS] + [pl.BlockSpec(memory_space=pltpu.HBM)] * len(tokens) + on_chip(heads + len(extra)),
        out_shape=f32(2 * side_rows, width),
        scratch_shapes=[
            pltpu.VMEM((2, 2, side_rows, feats), jnp.float32),
            pltpu.VMEM((2 * feats, width), jnp.bfloat16),
            pltpu.VMEM((2 * feats, width), jnp.bfloat16),
            pltpu.SemaphoreType.DMA((2, 2)),
        ],
        cost_estimate=pl.CostEstimate(
            flops=24 * side_rows * feats * width, bytes_accessed=16 * side_rows * feats, transcendentals=0
        ),
        name="project",
    )(at, *tokens, *weights, *extra)


def outward_kernel(heads, at_ref, *refs):
    pieces = refs[:heads]
    mine, sibling = refs[heads : heads + GROUPS], refs[heads + GROUPS : heads + 2 * GROUPS]
    outs = refs[heads + 2 * GROUPS : -2]
    top_ref, rem_ref = refs[-2:]
    s, h = at_ref[0], at_ref[1]
    j, m = s % heads, s // heads
    for far in range(heads):
        top, rem = halves(pieces[far][...])
        for slot in range(heads):

            @pl.when((j ^ far) == slot)
            def _():
                top_ref[:, slot * DK : (slot + 1) * DK] = top
                rem_ref[:, slot * DK : (slot + 1) * DK] = rem

    left = (top_ref[...], rem_ref[...])
    odd = s % 2 == 1
    for at in range(GROUPS):
        there = 2 * (m ^ (at >> 1)) + (at & 1)
        one = mul3(left, halves(mine[at][...]))
        two = mul3(left, halves(sibling[at][...]))
        width = one.shape[1]
        first = jnp.where(odd, two, one)
        second = jnp.where(odd, one, two)
        for g in range(GROUPS):

            @pl.when((h ^ g) == there)
            def _():
                outs[g][:, :width] = first
                outs[g][:, width:] = second


def outward(at, pieces, mine, sibling):
    heads = len(pieces)
    rows = pieces[0].shape[0]
    feats, width = mine[0].shape
    return pl.pallas_call(
        functools.partial(outward_kernel, heads),
        in_specs=[SCALARS] + on_chip(heads + 2 * GROUPS),
        scratch_shapes=[pltpu.VMEM((rows, feats), jnp.bfloat16)] * 2,
        out_shape=[f32(rows, 2 * width)] * GROUPS,
        cost_estimate=pl.CostEstimate(
            flops=12 * rows * feats * width * GROUPS, bytes_accessed=8 * GROUPS * feats * width, transcendentals=0
        ),
        name="outward",
    )(at, *pieces, *mine, *sibling)


def by_xor(shard, axis, with_):
    size = lax.axis_size(axis)
    return lax.ppermute(shard, axis, [(i, i ^ with_) for i in range(size)])


def exchanged(inputs, w_project, w_output, norm_gain):
    rows, _ = inputs.shape
    heads = w_project.shape[2] // DK
    seq = lax.axis_size("seq")
    spans = seq // heads
    s = lax.axis_index("seq")
    h = lax.axis_index("head")
    at = (jnp.arange(2, dtype=jnp.int32) * (h - s) + s).astype(jnp.int32)

    other = by_xor(inputs, "seq", 2)
    near_out = by_xor(w_output, "seq", 2)

    columns = head_columns(at, jnp.transpose(w_project, (1, 0, 2)))
    weights = [columns[far % heads] if far == 0 else by_xor(columns[far % heads], "seq", far) for far in range(seq)]

    own = jnp.concatenate([inputs, other], axis=0)
    mine = [own] + [by_xor(own, "head", g) for g in range(1, GROUPS)]
    siblings = [by_xor(piece, "seq", 1) for piece in mine]
    tokens = mine + siblings

    second = (s // 2) % 2 == 1
    pair = [jnp.where(second, near_out, w_output), jnp.where(second, w_output, near_out)]
    middle = [(i, i ^ 6) for i in range(seq) if i // 2 in (1, 2)]
    outer = [(i, i ^ 2) for i in range(seq) if i // 2 in (1, 2)]
    others = []
    for half in range(2):
        inner = lax.ppermute(pair[half], "seq", middle)
        others.append(inner + lax.ppermute(inner, "seq", outer))
    out_mine = pair + others
    out_sibling = [by_xor(w, "seq", 1) for w in out_mine]

    proj = None
    for span in range(spans):
        proj = project(at, tokens, weights[span * heads : (span + 1) * heads], span, proj)

    keys, w, u, leaving = chain_terms(proj)
    start = jnp.zeros((DK, DK), jnp.float32)
    for turn in range(spans - 1):
        if turn > 0:
            leaving = chain_leave(start, keys, w, u)
        start = from_behind(leaving, "seq", heads)
    normed = chain_output(start, proj, keys, w, u, norm_gain.reshape(heads, 1, DK), at, rows)

    pieces = [by_xor(piece, "seq", far) if far else piece for far, piece in enumerate(normed)]

    parts = outward(at, pieces, out_mine, out_sibling)
    total = parts[0]
    for g in range(1, GROUPS):
        total = total + by_xor(parts[g], "head", g)
    return total


def power_of_two(n):
    return n > 0 and n & (n - 1) == 0


def solution(mesh):
    seq, groups = mesh.shape["seq"], mesh.shape["head"]

    def step(inputs, w_project, w_output, norm_gain):
        heads = w_project.shape[2] // DK
        fits = (
            power_of_two(seq)
            and power_of_two(groups)
            and power_of_two(heads)
            and 2 <= heads <= seq
            and groups == GROUPS
            and heads == GROUPS
            and seq == 2 * GROUPS
            and w_project.shape[0] * 2 == inputs.shape[1]
            and w_project.shape[0] % 8 == 0
            and inputs.shape[0] == BLOCK
        )
        if not fits:
            return general(inputs, w_project, w_output, norm_gain)
        return exchanged(inputs, w_project, w_output, norm_gain)

    return jax.shard_map(
        step,
        mesh=mesh,
        in_specs=(P("seq", "head"), P("seq", None, "head"), P("head", "seq"), P("head")),
        out_specs=P("seq", "head"),
        check_vma=False,
    )
```

```python
import functools

import jax
import jax.numpy as jnp
from jax import lax
from jax.experimental import pallas as pl
from jax.experimental.pallas import tpu as pltpu
from jax.sharding import PartitionSpec as P


DK = 128
SPAN = 64
BLOCK = 256


HIGH = lax.Precision.HIGHEST


def from_behind(shard, axis, by):
    size = lax.axis_size(axis)
    pairs = [(i, i + by) for i in range(size) if 0 <= i + by < size]
    return lax.ppermute(shard, axis, pairs)


def unit_rows(matrix):
    return matrix * lax.rsqrt(jnp.sum(matrix * matrix, axis=-1, keepdims=True) + 1e-06)


def block_terms(queries, keys, values):
    width = keys.shape[-1]
    length = keys.shape[-2]
    inner = jnp.einsum("...ck,...dk->...cd", keys, keys, precision=HIGH)
    strict = jnp.tril(jnp.ones((length, length), jnp.float32), -1)
    system = jnp.eye(length, dtype=jnp.float32) + 2.0 * strict * inner
    stacked = 2.0 * jnp.concatenate([keys, values], axis=-1)
    solved = lax.linalg.triangular_solve(
        system, stacked, left_side=True, lower=True, unit_diagonal=True
    )
    w_rows = solved[..., :width]
    u_rows = solved[..., width:]
    transit = jnp.eye(width, dtype=jnp.float32) - jnp.einsum(
        "...cw,...ck->...wk", w_rows, keys, precision=HIGH
    )
    written = jnp.einsum("...cv,...ck->...vk", u_rows, keys, precision=HIGH)
    causal = jnp.tril(jnp.einsum("...ck,...dk->...cd", queries, keys, precision=HIGH))
    local_out = jnp.einsum("...cd,...dv->...cv", causal, u_rows, precision=HIGH)
    reach = queries - jnp.einsum("...cd,...dk->...ck", causal, w_rows, precision=HIGH)
    return (transit, written, local_out, reach)


def compose(first, second):
    return jnp.einsum("hvk,hkj->hvj", first, second, precision=HIGH)


def general(inputs, w_project, w_output, norm_gain):
    tok_rows = inputs.shape[0]
    columns = w_project.shape[2]
    heads = columns // DK
    blocks = tok_rows // SPAN
    features = lax.all_gather(inputs, "head", axis=1, tiled=True)
    proj = jnp.einsum(
        "td,dgc->tgc",
        features,
        lax.all_gather(w_project, "seq", axis=0, tiled=True),
        precision=HIGH,
    )
    proj = jnp.transpose(proj.reshape(blocks, SPAN, 3, heads, DK), (2, 0, 3, 1, 4))
    queries = unit_rows(proj[0])
    keys = unit_rows(proj[1])
    values = proj[2]
    transit, written, local_out, reach = block_terms(queries, keys, values)
    identity = jnp.broadcast_to(jnp.eye(DK, dtype=jnp.float32), (heads, DK, DK))
    nothing = jnp.zeros((heads, DK, DK), jnp.float32)

    def chain(carry, pair):
        acc_transit, acc_written = carry
        following = (compose(acc_transit, pair[0]), compose(acc_written, pair[0]) + pair[1])
        return (following, carry)

    (dev_transit, dev_written), (before_transit, before_written) = lax.scan(
        chain, (identity, nothing), (transit, written)
    )

    def relay_turn(turn, incoming):
        leaving = compose(incoming, dev_transit) + dev_written
        return from_behind(leaving, "seq", 1)

    entry = lax.fori_loop(0, lax.axis_size("seq") - 1, relay_turn, nothing)
    starts = jnp.einsum("hvk,nhkj->nhvj", entry, before_transit, precision=HIGH) + before_written
    outputs = local_out + jnp.einsum("nhck,nhvk->nhcv", reach, starts, precision=HIGH)
    outputs = jnp.transpose(outputs, (0, 2, 1, 3)).reshape(tok_rows, heads, DK)
    normed = outputs * lax.rsqrt(jnp.mean(outputs * outputs, axis=-1, keepdims=True) + 1e-06)
    normed = normed.reshape(tok_rows, heads * DK) * norm_gain
    partial_sums = jnp.dot(
        normed,
        lax.all_gather(w_output, "seq", axis=1, tiled=True),
        precision=HIGH,
        preferred_element_type=jnp.float32,
    )
    return lax.psum_scatter(partial_sums, "head", scatter_dimension=1, tiled=True)


def halves(a):
    top = a.astype(jnp.bfloat16)
    return top, (a - top.astype(jnp.float32)).astype(jnp.bfloat16)


def mul3(a, b, dims=((1,), (0,))):
    dot = functools.partial(
        lax.dot_general, dimension_numbers=(dims, ((), ())), preferred_element_type=jnp.float32
    )
    return dot(a[0], b[0]) + (dot(a[0], b[1]) + dot(a[1], b[0]))


def dot3(a, b, dims=((1,), (0,))):
    return mul3(halves(a), halves(b), dims)


def terms_kernel(proj_ref, keys_ref, w_ref, u_ref, end_ref, low_ref, inv_ref):
    groups = low_ref.shape[0]
    row = lax.broadcasted_iota(jnp.int32, (BLOCK, BLOCK), 0)
    col = lax.broadcasted_iota(jnp.int32, (BLOCK, BLOCK), 1)
    for n in range(groups):
        part = pl.ds(n * BLOCK, BLOCK)
        raw = proj_ref[part, DK : 2 * DK]
        keys = raw * lax.rsqrt(jnp.sum(raw * raw, axis=-1, keepdims=True) + 1e-06)
        keys_ref[part, :] = keys
        pair = halves(keys)
        low = jnp.where(row > col, 2.0 * mul3(pair, pair, ((1,), (1,))), 0.0)
        low_ref[n] = low
        inv_ref[n] = jnp.where(row == col, 1.0, jnp.where((row >> 1) == (col >> 1), -low, 0.0))

    def level(at, carry):
        here = ((row >> (at + 1)) == (col >> (at + 1))) & ((row >> at) != (col >> at))
        for n in range(groups):
            inverse = inv_ref[n]
            pair = halves(inverse)
            off = jnp.where(here, low_ref[n], 0.0)
            inv_ref[n] = inverse - mul3(pair, halves(mul3(halves(off), pair)))
        return carry

    lax.fori_loop(1, BLOCK.bit_length() - 1, level, 0)
    for n in range(groups):
        part = pl.ds(n * BLOCK, BLOCK)
        inverse = halves(inv_ref[n])
        w_ref[part, :] = mul3(inverse, halves(2.0 * keys_ref[part, :]))
        u_ref[part, :] = mul3(inverse, halves(2.0 * proj_ref[part, 2 * DK :]))
    state = jnp.zeros((DK, DK), jnp.float32)
    for n in range(groups):
        part = pl.ds(n * BLOCK, BLOCK)
        fresh = u_ref[part, :]
        if n > 0:
            fresh = fresh - dot3(w_ref[part, :], state)
        state = state + dot3(keys_ref[part, :], fresh, ((0,), (0,)))
    end_ref[...] = state


def leave_kernel(start_ref, keys_ref, w_ref, u_ref, end_ref):
    state = start_ref[...]
    for n in range(keys_ref.shape[0] // BLOCK):
        part = pl.ds(n * BLOCK, BLOCK)
        fresh = u_ref[part, :] - dot3(w_ref[part, :], state)
        state = state + dot3(keys_ref[part, :], fresh, ((0,), (0,)))
    end_ref[...] = state


def output_kernel(at_ref, start_ref, q_ref, keys_ref, w_ref, u_ref, gain_ref, *outs):
    heads = len(outs)
    j = at_ref[0] % heads
    gain = gain_ref[j]
    row = lax.broadcasted_iota(jnp.int32, (BLOCK, BLOCK), 0)
    col = lax.broadcasted_iota(jnp.int32, (BLOCK, BLOCK), 1)
    state = start_ref[...]
    for n in range(keys_ref.shape[0] // BLOCK):
        part = pl.ds(n * BLOCK, BLOCK)
        raw = q_ref[part, :DK]
        queries = halves(raw * lax.rsqrt(jnp.sum(raw * raw, axis=-1, keepdims=True) + 1e-06))
        keys = halves(keys_ref[part, :])
        causal = jnp.where(row >= col, mul3(queries, keys, ((1,), (1,))), 0.0)
        entry = halves(state)
        fresh = halves(u_ref[part, :] - mul3(halves(w_ref[part, :]), entry))
        result = mul3(queries, entry) + mul3(halves(causal), fresh)
        state = state + mul3(keys, fresh, ((0,), (0,)))
        result = result * lax.rsqrt(jnp.mean(result * result, axis=-1, keepdims=True) + 1e-06) * gain
        for far in range(heads):

            @pl.when((j ^ far) == n)
            def _():
                outs[far][...] = result


def f32(*shape):
    return pltpu.VMEM(shape, jnp.float32)


def bf16(*shape):
    return pltpu.VMEM(shape, jnp.bfloat16)


def on_chip(n):
    return [pl.BlockSpec(memory_space=pltpu.VMEM)] * n


def kept(arrays):
    return [pltpu.with_memory_space_constraint(a, pltpu.VMEM) for a in arrays]


SCALARS = pl.BlockSpec(memory_space=pltpu.SMEM)
GROUPS = 4
ROOM = pltpu.CompilerParams(vmem_limit_bytes=16 * 2**20)


def chain_terms(proj):
    rows = proj.shape[0]
    groups = rows // BLOCK
    flops = 3 * 2 * groups * BLOCK * BLOCK * BLOCK * 17
    return pl.pallas_call(
        terms_kernel,
        in_specs=on_chip(1),
        out_specs=on_chip(4),
        out_shape=(f32(rows, DK), f32(rows, DK), f32(rows, DK), f32(DK, DK)),
        scratch_shapes=[pltpu.VMEM((groups, BLOCK, BLOCK), jnp.float32)] * 2,
        cost_estimate=pl.CostEstimate(flops=flops, bytes_accessed=20 * rows * DK, transcendentals=rows),
        compiler_params=ROOM,
        name="chain_terms",
    )(*kept([proj]))


def chain_leave(start, keys, w, u):
    rows = keys.shape[0]
    return pl.pallas_call(
        leave_kernel,
        in_specs=on_chip(4),
        out_specs=on_chip(1)[0],
        out_shape=f32(DK, DK),
        cost_estimate=pl.CostEstimate(
            flops=3 * 4 * rows * DK * DK, bytes_accessed=12 * rows * DK, transcendentals=0
        ),
        compiler_params=ROOM,
        name="chain_leave",
    )(*kept([start, keys, w, u]))


def chain_output(start, proj, keys, w, u, gain, at, token_rows):
    rows = keys.shape[0]
    heads = rows // token_rows
    return pl.pallas_call(
        output_kernel,
        in_specs=[SCALARS] + on_chip(6),
        out_specs=on_chip(heads),
        out_shape=[f32(token_rows, DK)] * heads,
        cost_estimate=pl.CostEstimate(
            flops=3 * 2 * rows * DK * (3 * DK + 2 * BLOCK), bytes_accessed=20 * rows * DK, transcendentals=2 * rows
        ),
        compiler_params=ROOM,
        name="chain_output",
    )(at, *kept([start, proj, keys, w, u, gain]))


def columns_kernel(at_ref, w_ref, *outs):
    heads = len(outs)
    mine = at_ref[0] % heads
    for near in range(heads):
        for slot in range(heads):

            @pl.when((mine ^ near) == slot)
            def _():
                for part in range(w_ref.shape[0]):
                    outs[near][:, part * DK : (part + 1) * DK] = w_ref[part, :, slot * DK : (slot + 1) * DK]


def head_columns(at, w):
    parts, rows, width = w.shape
    return pl.pallas_call(
        columns_kernel,
        in_specs=[SCALARS] + on_chip(1),
        out_specs=on_chip(width // DK),
        out_shape=[f32(rows, parts * DK)] * (width // DK),
        compiler_params=ROOM,
        name="head_columns",
    )(at, w)


GROUPS = 4


def spread_kernel(at_ref, *refs):
    top_ref, rem_ref = refs[-2:]
    rows = refs[0].shape[0]
    for n, piece in enumerate(refs[:-2]):
        to = at_ref[1] ^ (n % GROUPS)
        part = pl.ds(n // GROUPS * rows, rows)
        top_ref[to, part, :], rem_ref[to, part, :] = halves(piece[...])


def spread(at, pieces):
    rows, feats = pieces[0].shape
    whole = (GROUPS, len(pieces) // GROUPS * rows, feats)
    return pl.pallas_call(
        spread_kernel,
        in_specs=[SCALARS] + on_chip(len(pieces)),
        out_specs=on_chip(2),
        out_shape=[bf16(*whole)] * 2,
        compiler_params=ROOM,
        name="spread",
    )(at, *kept(pieces))


def project_kernel(at_ref, *refs):
    tokens, weights, before = refs[:4], refs[4:6], refs[6:-5]
    out_ref, kv_top_ref, kv_rem_ref, q_both_ref, q_top_ref = refs[-5:]
    s, pair = at_ref[0], at_ref[2]
    j, z = s % GROUPS, s // 2
    rows = tokens[0].shape[1] // 2
    w_rows = weights[0].shape[0]
    for low in range(2):
        to = pl.ds(pl.multiple_of(((s & 1) ^ low) * w_rows, w_rows), w_rows)
        q_top, q_rem = halves(weights[low][:, :DK])
        q_top_ref[to, :] = q_top
        q_both_ref[to, :DK] = q_top
        q_both_ref[to, DK:] = q_rem
        kv_top_ref[to, :], kv_rem_ref[to, :] = halves(weights[low][:, DK:])
    dot = functools.partial(jnp.dot, preferred_element_type=jnp.float32)
    for at in range(4):
        to = pl.ds(pl.multiple_of((j ^ at) * rows, rows), rows)
        part = slice((at % 2) * rows, (at % 2 + 1) * rows)
        top, rem = tokens[at // 2 * 2][z ^ pair, part, :], tokens[at // 2 * 2 + 1][z ^ pair, part, :]
        kv = dot(top, kv_top_ref[...]) + (dot(top, kv_rem_ref[...]) + dot(rem, kv_top_ref[...]))
        both = dot(top, q_both_ref[...])
        q = both[:, :DK] + (both[:, DK:] + dot(rem, q_top_ref[...]))
        if before:
            kv = kv + before[0][to, DK:]
            q = q + before[0][to, :DK]
        out_ref[to, :DK] = q
        out_ref[to, DK:] = kv


def project(at, tokens, weights, before=None):
    _, two_rows, feats = tokens[0].shape
    _, width = weights[0].shape
    extra = [] if before is None else [before]
    rows = 2 * two_rows
    return pl.pallas_call(
        project_kernel,
        in_specs=[SCALARS] + on_chip(6 + len(extra)),
        out_specs=on_chip(1)[0],
        out_shape=f32(rows, width),
        scratch_shapes=[
            pltpu.VMEM((feats, width - DK), jnp.bfloat16),
            pltpu.VMEM((feats, width - DK), jnp.bfloat16),
            pltpu.VMEM((feats, 2 * DK), jnp.bfloat16),
            pltpu.VMEM((feats, DK), jnp.bfloat16),
        ],
        cost_estimate=pl.CostEstimate(
            flops=6 * rows * feats * width, bytes_accessed=4 * rows * feats, transcendentals=0
        ),
        compiler_params=ROOM,
        name="project",
    )(at, *kept([*tokens, *weights, *extra]))


def outward_kernel(heads, at_ref, *refs):
    pieces = refs[:heads]
    mine, sibling = refs[heads : heads + GROUPS], refs[heads + GROUPS : heads + 2 * GROUPS]
    outs = refs[heads + 2 * GROUPS : -2]
    top_ref, rem_ref = refs[-2:]
    s, h = at_ref[0], at_ref[1]
    j = s % heads
    for far in range(heads):
        top, rem = halves(pieces[far][...])
        for slot in range(heads):

            @pl.when((j ^ far) == slot)
            def _():
                top_ref[:, slot * DK : (slot + 1) * DK] = top
                rem_ref[:, slot * DK : (slot + 1) * DK] = rem

    left = (top_ref[...], rem_ref[...])
    odd = s % 2 == 1
    for at in range(GROUPS):
        there = (s // 2 - at) % GROUPS
        one = mul3(left, halves(mine[at][...]))
        two = mul3(left, halves(sibling[at][...]))
        width = one.shape[1]
        first = jnp.where(odd, two, one)
        second = jnp.where(odd, one, two)
        for g in range(GROUPS):

            @pl.when((h ^ g) == there)
            def _():
                outs[g][:, :width] = first
                outs[g][:, width:] = second


def outward(at, pieces, mine, sibling):
    heads = len(pieces)
    rows = pieces[0].shape[0]
    feats, width = mine[0].shape
    return pl.pallas_call(
        functools.partial(outward_kernel, heads),
        in_specs=[SCALARS] + on_chip(heads + 2 * GROUPS),
        out_specs=on_chip(GROUPS),
        compiler_params=ROOM,
        scratch_shapes=[pltpu.VMEM((rows, feats), jnp.bfloat16)] * 2,
        out_shape=[f32(rows, 2 * width)] * GROUPS,
        cost_estimate=pl.CostEstimate(
            flops=12 * rows * feats * width * GROUPS, bytes_accessed=8 * GROUPS * feats * width, transcendentals=0
        ),
        name="outward",
    )(at, *kept([*pieces, *mine, *sibling]))


def by_xor(shard, axis, with_):
    size = lax.axis_size(axis)
    return lax.ppermute(shard, axis, [(i, i ^ with_) for i in range(size)])


def exchanged(inputs, w_project, w_output, norm_gain):
    rows, _ = inputs.shape
    heads = w_project.shape[2] // DK
    seq = lax.axis_size("seq")
    spans = seq // heads
    s = lax.axis_index("seq")
    h = lax.axis_index("head")
    first = jnp.arange(3, dtype=jnp.int32)
    at = (jnp.where(first == 0, s, 0) + jnp.where(first == 1, h, 0)).astype(jnp.int32)

    other = by_xor(inputs, "seq", 2)

    columns = head_columns(at, jnp.transpose(w_project, (1, 0, 2)))
    weights = [columns[far % heads] if far == 0 else by_xor(columns[far % heads], "seq", far) for far in range(seq)]

    blocks = [None] * heads
    for far, block in ((0, inputs), (2, other)):
        blocks[far] = [block] + [by_xor(block, "head", g) for g in range(1, GROUPS)]
        blocks[far + 1] = [by_xor(piece, "seq", 1) for piece in blocks[far]]
    tokens = []
    for n in range(0, heads, 2):
        tokens += spread(at, blocks[n] + blocks[n + 1])

    proj = None
    for pair in range(seq // 2):
        where = at + jnp.array([0, 0, pair], jnp.int32)
        proj = project(where, tokens, weights[2 * pair : 2 * pair + 2], proj)

    right, left = w_output, w_output
    rights, lefts = [], []
    for _ in range(GROUPS - 1):
        right = lax.ppermute(right, "seq", [(i, i + 2) for i in range(seq - 2)])
        left = lax.ppermute(left, "seq", [(i + 2, i) for i in range(seq - 2)])
        rights.append(right)
        lefts.append(left)
    z = s // 2
    line = [w_output]
    for by in range(1, GROUPS):
        line.append(jnp.where(z >= by, rights[by - 1], lefts[GROUPS - 1 - by]))
    out_mine = line
    out_sibling = [by_xor(w, "seq", 1) for w in out_mine]

    keys, w, u, leaving = chain_terms(proj)
    start = jnp.zeros((DK, DK), jnp.float32)
    for turn in range(spans - 1):
        if turn > 0:
            leaving = chain_leave(start, keys, w, u)
        start = from_behind(leaving, "seq", heads)
    normed = chain_output(start, proj, keys, w, u, norm_gain.reshape(heads, 1, DK), at, rows)

    pieces = [by_xor(piece, "seq", far) if far else piece for far, piece in enumerate(normed)]

    parts = outward(at, pieces, out_mine, out_sibling)
    total = parts[0]
    for g in range(1, GROUPS):
        total = total + by_xor(parts[g], "head", g)
    return total


def power_of_two(n):
    return n > 0 and n & (n - 1) == 0


def solution(mesh):
    seq, groups = mesh.shape["seq"], mesh.shape["head"]

    def step(inputs, w_project, w_output, norm_gain):
        heads = w_project.shape[2] // DK
        fits = (
            power_of_two(seq)
            and power_of_two(groups)
            and power_of_two(heads)
            and 2 <= heads <= seq
            and groups == GROUPS
            and heads == GROUPS
            and seq == 2 * GROUPS
            and w_project.shape[0] * 2 == inputs.shape[1]
            and w_project.shape[0] % 8 == 0
            and inputs.shape[0] == BLOCK
        )
        if not fits:
            return general(inputs, w_project, w_output, norm_gain)
        return exchanged(inputs, w_project, w_output, norm_gain)

    return jax.shard_map(
        step,
        mesh=mesh,
        in_specs=(P("seq", "head"), P("seq", None, "head"), P("head", "seq"), P("head")),
        out_specs=P("seq", "head"),
        check_vma=False,
    )
```

```python
import functools

import jax
import jax.numpy as jnp
from jax import lax
from jax.experimental import pallas as pl
from jax.experimental.pallas import tpu as pltpu
from jax.sharding import PartitionSpec as P


DK = 128
SPAN = 64
BLOCK = 256


HIGH = lax.Precision.HIGHEST


def from_behind(shard, axis, by):
    size = lax.axis_size(axis)
    pairs = [(i, i + by) for i in range(size) if 0 <= i + by < size]
    return lax.ppermute(shard, axis, pairs)


def unit_rows(matrix):
    return matrix * lax.rsqrt(jnp.sum(matrix * matrix, axis=-1, keepdims=True) + 1e-06)


def block_terms(queries, keys, values):
    width = keys.shape[-1]
    length = keys.shape[-2]
    inner = jnp.einsum("...ck,...dk->...cd", keys, keys, precision=HIGH)
    strict = jnp.tril(jnp.ones((length, length), jnp.float32), -1)
    system = jnp.eye(length, dtype=jnp.float32) + 2.0 * strict * inner
    stacked = 2.0 * jnp.concatenate([keys, values], axis=-1)
    solved = lax.linalg.triangular_solve(
        system, stacked, left_side=True, lower=True, unit_diagonal=True
    )
    w_rows = solved[..., :width]
    u_rows = solved[..., width:]
    transit = jnp.eye(width, dtype=jnp.float32) - jnp.einsum(
        "...cw,...ck->...wk", w_rows, keys, precision=HIGH
    )
    written = jnp.einsum("...cv,...ck->...vk", u_rows, keys, precision=HIGH)
    causal = jnp.tril(jnp.einsum("...ck,...dk->...cd", queries, keys, precision=HIGH))
    local_out = jnp.einsum("...cd,...dv->...cv", causal, u_rows, precision=HIGH)
    reach = queries - jnp.einsum("...cd,...dk->...ck", causal, w_rows, precision=HIGH)
    return (transit, written, local_out, reach)


def compose(first, second):
    return jnp.einsum("hvk,hkj->hvj", first, second, precision=HIGH)


def general(inputs, w_project, w_output, norm_gain):
    tok_rows = inputs.shape[0]
    columns = w_project.shape[2]
    heads = columns // DK
    blocks = tok_rows // SPAN
    features = lax.all_gather(inputs, "head", axis=1, tiled=True)
    proj = jnp.einsum(
        "td,dgc->tgc",
        features,
        lax.all_gather(w_project, "seq", axis=0, tiled=True),
        precision=HIGH,
    )
    proj = jnp.transpose(proj.reshape(blocks, SPAN, 3, heads, DK), (2, 0, 3, 1, 4))
    queries = unit_rows(proj[0])
    keys = unit_rows(proj[1])
    values = proj[2]
    transit, written, local_out, reach = block_terms(queries, keys, values)
    identity = jnp.broadcast_to(jnp.eye(DK, dtype=jnp.float32), (heads, DK, DK))
    nothing = jnp.zeros((heads, DK, DK), jnp.float32)

    def chain(carry, pair):
        acc_transit, acc_written = carry
        following = (compose(acc_transit, pair[0]), compose(acc_written, pair[0]) + pair[1])
        return (following, carry)

    (dev_transit, dev_written), (before_transit, before_written) = lax.scan(
        chain, (identity, nothing), (transit, written)
    )

    def relay_turn(turn, incoming):
        leaving = compose(incoming, dev_transit) + dev_written
        return from_behind(leaving, "seq", 1)

    entry = lax.fori_loop(0, lax.axis_size("seq") - 1, relay_turn, nothing)
    starts = jnp.einsum("hvk,nhkj->nhvj", entry, before_transit, precision=HIGH) + before_written
    outputs = local_out + jnp.einsum("nhck,nhvk->nhcv", reach, starts, precision=HIGH)
    outputs = jnp.transpose(outputs, (0, 2, 1, 3)).reshape(tok_rows, heads, DK)
    normed = outputs * lax.rsqrt(jnp.mean(outputs * outputs, axis=-1, keepdims=True) + 1e-06)
    normed = normed.reshape(tok_rows, heads * DK) * norm_gain
    partial_sums = jnp.dot(
        normed,
        lax.all_gather(w_output, "seq", axis=1, tiled=True),
        precision=HIGH,
        preferred_element_type=jnp.float32,
    )
    return lax.psum_scatter(partial_sums, "head", scatter_dimension=1, tiled=True)


def halves(a):
    top = a.astype(jnp.bfloat16)
    return top, (a - top.astype(jnp.float32)).astype(jnp.bfloat16)


def mul3(a, b, dims=((1,), (0,))):
    dot = functools.partial(
        lax.dot_general, dimension_numbers=(dims, ((), ())), preferred_element_type=jnp.float32
    )
    return dot(a[0], b[0]) + (dot(a[0], b[1]) + dot(a[1], b[0]))


def dot3(a, b, dims=((1,), (0,))):
    return mul3(halves(a), halves(b), dims)


def thirds(a):
    top = a.astype(jnp.bfloat16)
    rest = a - top.astype(jnp.float32)
    mid = rest.astype(jnp.bfloat16)
    return top, mid, (rest - mid.astype(jnp.float32)).astype(jnp.bfloat16)


def beside(*parts):
    return jnp.concatenate(parts, axis=1)


def above(*parts):
    return jnp.concatenate(parts, axis=0)


def product(a, b):
    return jnp.dot(a, b, preferred_element_type=jnp.float32)


def square3(a, b):
    both = product(beside(*a), above(beside(*b), beside(b[0], jnp.zeros_like(b[0]))))
    return both[:, : both.shape[1] // 2] + both[:, both.shape[1] // 2 :]


def wide3(a, b):
    return product(beside(*a), above(b[0], b[0])) + product(a[0], b[1])


def square6(a, b):
    pair = beside(b[0], b[1])
    both = product(beside(a[0], a[1]), above(pair, pair))
    small = product(beside(a[0], a[2]), above(b[2], b[0]))
    return both[:, : both.shape[1] // 2] + (both[:, both.shape[1] // 2 :] + small)


def wide6(a, b):
    front = beside(a[0], a[1])
    small = product(front, above(b[1], b[1])) + product(beside(a[0], a[2]), above(b[2], b[0]))
    return product(front, above(b[0], b[0])) + small


def terms_kernel(proj_ref, keys_ref, w_ref, u_ref, end_ref, low_ref, cross_ref, inv_ref):
    count, size, _ = low_ref.shape
    row = lax.broadcasted_iota(jnp.int32, (size, size), 0)
    col = lax.broadcasted_iota(jnp.int32, (size, size), 1)
    one = jnp.where(row == col, 1.0, 0.0)
    for n in range(count // 2):
        part = slice(n * BLOCK, (n + 1) * BLOCK)
        raw = proj_ref[part, DK : 2 * DK]
        keys = raw * lax.rsqrt(jnp.sum(raw * raw, axis=-1, keepdims=True) + 1e-06)
        keys_ref[part, :] = keys
        top, rem = halves(keys)
        gram = lax.dot_general(
            beside(top, rem), beside(top, top), (((1,), (1,)), ((), ())), preferred_element_type=jnp.float32
        ) + lax.dot_general(top, rem, (((1,), (1,)), ((), ())), preferred_element_type=jnp.float32)
        gram = gram + gram
        cross_ref[n] = gram[size:, :size]
        for half in range(2):
            low = jnp.where(row > col, gram[half * size : (half + 1) * size, half * size : (half + 1) * size], 0.0)
            low_ref[2 * n + half] = low
            inv_ref[2 * n + half] = one - jnp.where((row >> 1) == (col >> 1), low, 0.0)

    def level(at, carry):
        here = ((row >> (at + 1)) == (col >> (at + 1))) & ((row >> at) != (col >> at))
        for n in range(count):
            inverse = inv_ref[n]
            coarse = inverse.astype(jnp.bfloat16)
            off = jnp.where(here, low_ref[n], 0.0).astype(jnp.bfloat16)
            inv_ref[n] = inverse - product(coarse, product(off, coarse).astype(jnp.bfloat16))
        return carry

    lax.fori_loop(1, size.bit_length() - 1, level, 0)
    for n in range(count):
        inverse = inv_ref[n]
        pair = halves(inverse)
        error = (one - inverse) - square3(halves(low_ref[n]), pair)
        inv_ref[n] = inverse + product(pair[0], error.astype(jnp.bfloat16))
    for n in range(count):
        inverse = inv_ref[n]
        parts = thirds(inverse)
        error = (one - inverse) - square6(thirds(low_ref[n]), parts)
        inv_ref[n] = inverse + square3(parts[:2], halves(error))

    def given(n):
        part = slice(n * size, (n + 1) * size)
        return 2.0 * beside(keys_ref[part, :], proj_ref[part, 2 * DK :])

    for n in range(count // 2):
        first = wide3(halves(inv_ref[2 * n]), halves(given(2 * n)))
        later = given(2 * n + 1) - wide6(thirds(cross_ref[n]), thirds(first))
        second = wide3(halves(inv_ref[2 * n + 1]), halves(later))
        for at, found in ((2 * n, first), (2 * n + 1, second)):
            part = slice(at * size, (at + 1) * size)
            w_ref[part, :] = found[:, :DK]
            u_ref[part, :] = found[:, DK:]
    state = jnp.zeros((DK, DK), jnp.float32)
    for n in range(count // 2):
        part = slice(n * BLOCK, (n + 1) * BLOCK)
        fresh = u_ref[part, :]
        if n > 0:
            fresh = fresh - square3(halves(w_ref[part, :]), halves(state))
        state = state + dot3(keys_ref[part, :], fresh, ((0,), (0,)))
    end_ref[...] = state


def leave_kernel(start_ref, keys_ref, w_ref, u_ref, end_ref):
    state = start_ref[...]
    for n in range(keys_ref.shape[0] // BLOCK):
        part = pl.ds(n * BLOCK, BLOCK)
        fresh = u_ref[part, :] - dot3(w_ref[part, :], state)
        state = state + dot3(keys_ref[part, :], fresh, ((0,), (0,)))
    end_ref[...] = state


def output_kernel(at_ref, start_ref, q_ref, keys_ref, w_ref, u_ref, gain_ref, *outs):
    heads = len(outs)
    j = at_ref[0] % heads
    gain = gain_ref[j]
    row = lax.broadcasted_iota(jnp.int32, (BLOCK, BLOCK), 0)
    col = lax.broadcasted_iota(jnp.int32, (BLOCK, BLOCK), 1)
    state = start_ref[...]
    for n in range(keys_ref.shape[0] // BLOCK):
        part = pl.ds(n * BLOCK, BLOCK)
        raw = q_ref[part, :DK]
        queries = halves(raw * lax.rsqrt(jnp.sum(raw * raw, axis=-1, keepdims=True) + 1e-06))
        keys = halves(keys_ref[part, :])
        causal = jnp.where(row >= col, mul3(queries, keys, ((1,), (1,))), 0.0)
        entry = halves(state)
        fresh = halves(u_ref[part, :] - mul3(halves(w_ref[part, :]), entry))
        result = mul3(queries, entry) + mul3(halves(causal), fresh)
        state = state + mul3(keys, fresh, ((0,), (0,)))
        result = result * lax.rsqrt(jnp.mean(result * result, axis=-1, keepdims=True) + 1e-06) * gain
        for far in range(heads):

            @pl.when((j ^ far) == n)
            def _():
                outs[far][...] = result


def f32(*shape):
    return pltpu.VMEM(shape, jnp.float32)


def bf16(*shape):
    return pltpu.VMEM(shape, jnp.bfloat16)


def on_chip(n):
    return [pl.BlockSpec(memory_space=pltpu.VMEM)] * n


def kept(arrays):
    return [pltpu.with_memory_space_constraint(a, pltpu.VMEM) for a in arrays]


SCALARS = pl.BlockSpec(memory_space=pltpu.SMEM)
GROUPS = 4
ROOM = pltpu.CompilerParams(vmem_limit_bytes=16 * 2**20)


def chain_terms(proj):
    rows = proj.shape[0]
    groups = rows // BLOCK
    flops = 3 * 2 * groups * BLOCK * BLOCK * BLOCK * 17
    return pl.pallas_call(
        terms_kernel,
        in_specs=on_chip(1),
        out_specs=on_chip(4),
        out_shape=(f32(rows, DK), f32(rows, DK), f32(rows, DK), f32(DK, DK)),
        scratch_shapes=[
            pltpu.VMEM((count, BLOCK // 2, BLOCK // 2), jnp.float32) for count in (2 * groups, groups, 2 * groups)
        ],
        cost_estimate=pl.CostEstimate(flops=flops, bytes_accessed=20 * rows * DK, transcendentals=rows),
        compiler_params=ROOM,
        name="chain_terms",
    )(*kept([proj]))


def chain_leave(start, keys, w, u):
    rows = keys.shape[0]
    return pl.pallas_call(
        leave_kernel,
        in_specs=on_chip(4),
        out_specs=on_chip(1)[0],
        out_shape=f32(DK, DK),
        cost_estimate=pl.CostEstimate(
            flops=3 * 4 * rows * DK * DK, bytes_accessed=12 * rows * DK, transcendentals=0
        ),
        compiler_params=ROOM,
        name="chain_leave",
    )(*kept([start, keys, w, u]))


def chain_output(start, proj, keys, w, u, gain, at, token_rows):
    rows = keys.shape[0]
    heads = rows // token_rows
    return pl.pallas_call(
        output_kernel,
        in_specs=[SCALARS] + on_chip(6),
        out_specs=on_chip(heads),
        out_shape=[f32(token_rows, DK)] * heads,
        cost_estimate=pl.CostEstimate(
            flops=3 * 2 * rows * DK * (3 * DK + 2 * BLOCK), bytes_accessed=20 * rows * DK, transcendentals=2 * rows
        ),
        compiler_params=ROOM,
        name="chain_output",
    )(at, *kept([start, proj, keys, w, u, gain]))


def columns_kernel(at_ref, w_ref, *outs):
    heads = len(outs)
    mine = at_ref[0] % heads
    for near in range(heads):
        for slot in range(heads):

            @pl.when((mine ^ near) == slot)
            def _():
                for part in range(w_ref.shape[0]):
                    outs[near][:, part * DK : (part + 1) * DK] = w_ref[part, :, slot * DK : (slot + 1) * DK]


def head_columns(at, w):
    parts, rows, width = w.shape
    return pl.pallas_call(
        columns_kernel,
        in_specs=[SCALARS] + on_chip(1),
        out_specs=on_chip(width // DK),
        out_shape=[f32(rows, parts * DK)] * (width // DK),
        compiler_params=ROOM,
        name="head_columns",
    )(at, w)


GROUPS = 4


def spread_kernel(at_ref, *refs):
    top_ref, rem_ref = refs[-2:]
    rows = refs[0].shape[0]
    for n, piece in enumerate(refs[:-2]):
        to = at_ref[1] ^ (n % GROUPS)
        part = pl.ds(n // GROUPS * rows, rows)
        top_ref[to, part, :], rem_ref[to, part, :] = halves(piece[...])


def spread(at, pieces):
    rows, feats = pieces[0].shape
    whole = (GROUPS, len(pieces) // GROUPS * rows, feats)
    return pl.pallas_call(
        spread_kernel,
        in_specs=[SCALARS] + on_chip(len(pieces)),
        out_specs=on_chip(2),
        out_shape=[bf16(*whole)] * 2,
        compiler_params=ROOM,
        name="spread",
    )(at, *kept(pieces))


def project_kernel(at_ref, *refs):
    tokens, weights, before = refs[:4], refs[4:6], refs[6:-5]
    out_ref, kv_top_ref, kv_rem_ref, q_both_ref, q_top_ref = refs[-5:]
    s, pair = at_ref[0], at_ref[2]
    j, z = s % GROUPS, s // 2
    rows = tokens[0].shape[1] // 2
    w_rows = weights[0].shape[0]
    for low in range(2):
        to = pl.ds(pl.multiple_of(((s & 1) ^ low) * w_rows, w_rows), w_rows)
        q_top, q_rem = halves(weights[low][:, :DK])
        q_top_ref[to, :] = q_top
        q_both_ref[to, :DK] = q_top
        q_both_ref[to, DK:] = q_rem
        kv_top_ref[to, :], kv_rem_ref[to, :] = halves(weights[low][:, DK:])
    dot = functools.partial(jnp.dot, preferred_element_type=jnp.float32)
    for at in range(4):
        to = pl.ds(pl.multiple_of((j ^ at) * rows, rows), rows)
        part = slice((at % 2) * rows, (at % 2 + 1) * rows)
        top, rem = tokens[at // 2 * 2][z ^ pair, part, :], tokens[at // 2 * 2 + 1][z ^ pair, part, :]
        kv = dot(top, kv_top_ref[...]) + (dot(top, kv_rem_ref[...]) + dot(rem, kv_top_ref[...]))
        both = dot(top, q_both_ref[...])
        q = both[:, :DK] + (both[:, DK:] + dot(rem, q_top_ref[...]))
        if before:
            kv = kv + before[0][to, DK:]
            q = q + before[0][to, :DK]
        out_ref[to, :DK] = q
        out_ref[to, DK:] = kv


def project(at, tokens, weights, before=None):
    _, two_rows, feats = tokens[0].shape
    _, width = weights[0].shape
    extra = [] if before is None else [before]
    rows = 2 * two_rows
    return pl.pallas_call(
        project_kernel,
        in_specs=[SCALARS] + on_chip(6 + len(extra)),
        out_specs=on_chip(1)[0],
        out_shape=f32(rows, width),
        scratch_shapes=[
            pltpu.VMEM((feats, width - DK), jnp.bfloat16),
            pltpu.VMEM((feats, width - DK), jnp.bfloat16),
            pltpu.VMEM((feats, 2 * DK), jnp.bfloat16),
            pltpu.VMEM((feats, DK), jnp.bfloat16),
        ],
        cost_estimate=pl.CostEstimate(
            flops=6 * rows * feats * width, bytes_accessed=4 * rows * feats, transcendentals=0
        ),
        compiler_params=ROOM,
        name="project",
    )(at, *kept([*tokens, *weights, *extra]))


def outward_kernel(heads, at_ref, *refs):
    pieces = refs[:heads]
    mine, sibling = refs[heads : heads + GROUPS], refs[heads + GROUPS : heads + 2 * GROUPS]
    outs = refs[heads + 2 * GROUPS : -2]
    top_ref, rem_ref = refs[-2:]
    s, h = at_ref[0], at_ref[1]
    j = s % heads
    for far in range(heads):
        top, rem = halves(pieces[far][...])
        for slot in range(heads):

            @pl.when((j ^ far) == slot)
            def _():
                top_ref[:, slot * DK : (slot + 1) * DK] = top
                rem_ref[:, slot * DK : (slot + 1) * DK] = rem

    left = (top_ref[...], rem_ref[...])
    odd = s % 2 == 1
    for at in range(GROUPS):
        there = (s // 2 - at) % GROUPS
        one = mul3(left, halves(mine[at][...]))
        two = mul3(left, halves(sibling[at][...]))
        width = one.shape[1]
        first = jnp.where(odd, two, one)
        second = jnp.where(odd, one, two)
        for g in range(GROUPS):

            @pl.when((h ^ g) == there)
            def _():
                outs[g][:, :width] = first
                outs[g][:, width:] = second


def outward(at, pieces, mine, sibling):
    heads = len(pieces)
    rows = pieces[0].shape[0]
    feats, width = mine[0].shape
    return pl.pallas_call(
        functools.partial(outward_kernel, heads),
        in_specs=[SCALARS] + on_chip(heads + 2 * GROUPS),
        out_specs=on_chip(GROUPS),
        compiler_params=ROOM,
        scratch_shapes=[pltpu.VMEM((rows, feats), jnp.bfloat16)] * 2,
        out_shape=[f32(rows, 2 * width)] * GROUPS,
        cost_estimate=pl.CostEstimate(
            flops=12 * rows * feats * width * GROUPS, bytes_accessed=8 * GROUPS * feats * width, transcendentals=0
        ),
        name="outward",
    )(at, *kept([*pieces, *mine, *sibling]))


def by_xor(shard, axis, with_):
    size = lax.axis_size(axis)
    return lax.ppermute(shard, axis, [(i, i ^ with_) for i in range(size)])


def exchanged(inputs, w_project, w_output, norm_gain):
    rows, _ = inputs.shape
    heads = w_project.shape[2] // DK
    seq = lax.axis_size("seq")
    spans = seq // heads
    s = lax.axis_index("seq")
    h = lax.axis_index("head")
    first = jnp.arange(3, dtype=jnp.int32)
    at = (jnp.where(first == 0, s, 0) + jnp.where(first == 1, h, 0)).astype(jnp.int32)

    other = by_xor(inputs, "seq", 2)

    columns = head_columns(at, jnp.transpose(w_project, (1, 0, 2)))
    weights = [columns[far % heads] if far == 0 else by_xor(columns[far % heads], "seq", far) for far in range(seq)]

    blocks = [None] * heads
    for far, block in ((0, inputs), (2, other)):
        blocks[far] = [block] + [by_xor(block, "head", g) for g in range(1, GROUPS)]
        blocks[far + 1] = [by_xor(piece, "seq", 1) for piece in blocks[far]]
    tokens = []
    for n in range(0, heads, 2):
        tokens += spread(at, blocks[n] + blocks[n + 1])

    proj = None
    for pair in range(seq // 2):
        where = at + jnp.array([0, 0, pair], jnp.int32)
        proj = project(where, tokens, weights[2 * pair : 2 * pair + 2], proj)

    right, left = w_output, w_output
    rights, lefts = [], []
    for _ in range(GROUPS - 1):
        right = lax.ppermute(right, "seq", [(i, i + 2) for i in range(seq - 2)])
        left = lax.ppermute(left, "seq", [(i + 2, i) for i in range(seq - 2)])
        rights.append(right)
        lefts.append(left)
    z = s // 2
    line = [w_output]
    for by in range(1, GROUPS):
        line.append(jnp.where(z >= by, rights[by - 1], lefts[GROUPS - 1 - by]))
    out_mine = line
    out_sibling = [by_xor(w, "seq", 1) for w in out_mine]

    keys, w, u, leaving = chain_terms(proj)
    start = jnp.zeros((DK, DK), jnp.float32)
    for turn in range(spans - 1):
        if turn > 0:
            leaving = chain_leave(start, keys, w, u)
        start = from_behind(leaving, "seq", heads)
    normed = chain_output(start, proj, keys, w, u, norm_gain.reshape(heads, 1, DK), at, rows)

    pieces = [by_xor(piece, "seq", far) if far else piece for far, piece in enumerate(normed)]

    parts = outward(at, pieces, out_mine, out_sibling)
    total = parts[0]
    for g in range(1, GROUPS):
        total = total + by_xor(parts[g], "head", g)
    return total


def power_of_two(n):
    return n > 0 and n & (n - 1) == 0


def solution(mesh):
    seq, groups = mesh.shape["seq"], mesh.shape["head"]

    def step(inputs, w_project, w_output, norm_gain):
        heads = w_project.shape[2] // DK
        fits = (
            power_of_two(seq)
            and power_of_two(groups)
            and power_of_two(heads)
            and 2 <= heads <= seq
            and groups == GROUPS
            and heads == GROUPS
            and seq == 2 * GROUPS
            and w_project.shape[0] * 2 == inputs.shape[1]
            and w_project.shape[0] % 8 == 0
            and inputs.shape[0] == BLOCK
        )
        if not fits:
            return general(inputs, w_project, w_output, norm_gain)
        return exchanged(inputs, w_project, w_output, norm_gain)

    return jax.shard_map(
        step,
        mesh=mesh,
        in_specs=(P("seq", "head"), P("seq", None, "head"), P("head", "seq"), P("head")),
        out_specs=P("seq", "head"),
        check_vma=False,
    )
```

```python
import functools

import jax
import jax.numpy as jnp
from jax import lax
from jax.experimental import pallas as pl
from jax.experimental.pallas import tpu as pltpu
from jax.sharding import PartitionSpec as P


DK = 128
SPAN = 64
BLOCK = 256


HIGH = lax.Precision.HIGHEST


def from_behind(shard, axis, by):
    size = lax.axis_size(axis)
    pairs = [(i, i + by) for i in range(size) if 0 <= i + by < size]
    return lax.ppermute(shard, axis, pairs)


def unit_rows(matrix):
    return matrix * lax.rsqrt(jnp.sum(matrix * matrix, axis=-1, keepdims=True) + 1e-06)


def block_terms(queries, keys, values):
    width = keys.shape[-1]
    length = keys.shape[-2]
    inner = jnp.einsum("...ck,...dk->...cd", keys, keys, precision=HIGH)
    strict = jnp.tril(jnp.ones((length, length), jnp.float32), -1)
    system = jnp.eye(length, dtype=jnp.float32) + 2.0 * strict * inner
    stacked = 2.0 * jnp.concatenate([keys, values], axis=-1)
    solved = lax.linalg.triangular_solve(
        system, stacked, left_side=True, lower=True, unit_diagonal=True
    )
    w_rows = solved[..., :width]
    u_rows = solved[..., width:]
    transit = jnp.eye(width, dtype=jnp.float32) - jnp.einsum(
        "...cw,...ck->...wk", w_rows, keys, precision=HIGH
    )
    written = jnp.einsum("...cv,...ck->...vk", u_rows, keys, precision=HIGH)
    causal = jnp.tril(jnp.einsum("...ck,...dk->...cd", queries, keys, precision=HIGH))
    local_out = jnp.einsum("...cd,...dv->...cv", causal, u_rows, precision=HIGH)
    reach = queries - jnp.einsum("...cd,...dk->...ck", causal, w_rows, precision=HIGH)
    return (transit, written, local_out, reach)


def compose(first, second):
    return jnp.einsum("hvk,hkj->hvj", first, second, precision=HIGH)


def general(inputs, w_project, w_output, norm_gain):
    tok_rows = inputs.shape[0]
    columns = w_project.shape[2]
    heads = columns // DK
    blocks = tok_rows // SPAN
    features = lax.all_gather(inputs, "head", axis=1, tiled=True)
    proj = jnp.einsum(
        "td,dgc->tgc",
        features,
        lax.all_gather(w_project, "seq", axis=0, tiled=True),
        precision=HIGH,
    )
    proj = jnp.transpose(proj.reshape(blocks, SPAN, 3, heads, DK), (2, 0, 3, 1, 4))
    queries = unit_rows(proj[0])
    keys = unit_rows(proj[1])
    values = proj[2]
    transit, written, local_out, reach = block_terms(queries, keys, values)
    identity = jnp.broadcast_to(jnp.eye(DK, dtype=jnp.float32), (heads, DK, DK))
    nothing = jnp.zeros((heads, DK, DK), jnp.float32)

    def chain(carry, pair):
        acc_transit, acc_written = carry
        following = (compose(acc_transit, pair[0]), compose(acc_written, pair[0]) + pair[1])
        return (following, carry)

    (dev_transit, dev_written), (before_transit, before_written) = lax.scan(
        chain, (identity, nothing), (transit, written)
    )

    def relay_turn(turn, incoming):
        leaving = compose(incoming, dev_transit) + dev_written
        return from_behind(leaving, "seq", 1)

    entry = lax.fori_loop(0, lax.axis_size("seq") - 1, relay_turn, nothing)
    starts = jnp.einsum("hvk,nhkj->nhvj", entry, before_transit, precision=HIGH) + before_written
    outputs = local_out + jnp.einsum("nhck,nhvk->nhcv", reach, starts, precision=HIGH)
    outputs = jnp.transpose(outputs, (0, 2, 1, 3)).reshape(tok_rows, heads, DK)
    normed = outputs * lax.rsqrt(jnp.mean(outputs * outputs, axis=-1, keepdims=True) + 1e-06)
    normed = normed.reshape(tok_rows, heads * DK) * norm_gain
    partial_sums = jnp.dot(
        normed,
        lax.all_gather(w_output, "seq", axis=1, tiled=True),
        precision=HIGH,
        preferred_element_type=jnp.float32,
    )
    return lax.psum_scatter(partial_sums, "head", scatter_dimension=1, tiled=True)


def halves(a):
    top = a.astype(jnp.bfloat16)
    return top, (a - top.astype(jnp.float32)).astype(jnp.bfloat16)


def mul3(a, b, dims=((1,), (0,))):
    dot = functools.partial(
        lax.dot_general, dimension_numbers=(dims, ((), ())), preferred_element_type=jnp.float32
    )
    return dot(a[0], b[0]) + (dot(a[0], b[1]) + dot(a[1], b[0]))


def dot3(a, b, dims=((1,), (0,))):
    return mul3(halves(a), halves(b), dims)


def thirds(a):
    top = a.astype(jnp.bfloat16)
    rest = a - top.astype(jnp.float32)
    mid = rest.astype(jnp.bfloat16)
    return top, mid, (rest - mid.astype(jnp.float32)).astype(jnp.bfloat16)


def beside(*parts):
    return jnp.concatenate(parts, axis=1)


def above(*parts):
    return jnp.concatenate(parts, axis=0)


def product(a, b):
    return jnp.dot(a, b, preferred_element_type=jnp.float32)


def square3(a, b):
    both = product(beside(*a), above(beside(*b), beside(b[0], jnp.zeros_like(b[0]))))
    return both[:, : both.shape[1] // 2] + both[:, both.shape[1] // 2 :]


def wide3(a, b):
    return product(beside(*a), above(b[0], b[0])) + product(a[0], b[1])


def square6(a, b):
    pair = beside(b[0], b[1])
    both = product(beside(a[0], a[1]), above(pair, pair))
    small = product(beside(a[0], a[2]), above(b[2], b[0]))
    return both[:, : both.shape[1] // 2] + (both[:, both.shape[1] // 2 :] + small)


def wide6(a, b):
    front = beside(a[0], a[1])
    small = product(front, above(b[1], b[1])) + product(beside(a[0], a[2]), above(b[2], b[0]))
    return product(front, above(b[0], b[0])) + small


def inverse_kernel(proj_ref, keys_ref, inv_ref, cross_ref, low_ref):
    count, size, _ = low_ref.shape
    row = lax.broadcasted_iota(jnp.int32, (size, size), 0)
    col = lax.broadcasted_iota(jnp.int32, (size, size), 1)
    one = jnp.where(row == col, 1.0, 0.0)
    for n in range(count // 2):
        part = slice(n * BLOCK, (n + 1) * BLOCK)
        raw = proj_ref[part, DK : 2 * DK]
        keys = raw * lax.rsqrt(jnp.sum(raw * raw, axis=-1, keepdims=True) + 1e-06)
        keys_ref[part, :] = keys
        top, rem = halves(keys)
        gram = lax.dot_general(
            beside(top, rem), beside(top, top), (((1,), (1,)), ((), ())), preferred_element_type=jnp.float32
        ) + lax.dot_general(top, rem, (((1,), (1,)), ((), ())), preferred_element_type=jnp.float32)
        gram = gram + gram
        cross_ref[n] = gram[size:, :size]
        for half in range(2):
            low = jnp.where(row > col, gram[half * size : (half + 1) * size, half * size : (half + 1) * size], 0.0)
            low_ref[2 * n + half] = low
            inv_ref[2 * n + half] = one - jnp.where((row >> 1) == (col >> 1), low, 0.0)

    def level(at, carry):
        here = ((row >> (at + 1)) == (col >> (at + 1))) & ((row >> at) != (col >> at))
        for n in range(count):
            inverse = inv_ref[n]
            coarse = inverse.astype(jnp.bfloat16)
            off = jnp.where(here, low_ref[n], 0.0).astype(jnp.bfloat16)
            inv_ref[n] = inverse - product(coarse, product(off, coarse).astype(jnp.bfloat16))
        return carry

    lax.fori_loop(1, size.bit_length() - 1, level, 0)
    for n in range(count):
        inverse = inv_ref[n]
        pair = halves(inverse)
        error = (one - inverse) - square3(halves(low_ref[n]), pair)
        inv_ref[n] = inverse + product(pair[0], error.astype(jnp.bfloat16))
    for n in range(count):
        inverse = inv_ref[n]
        parts = thirds(inverse)
        error = (one - inverse) - square6(thirds(low_ref[n]), parts)
        inv_ref[n] = inverse + square3(parts[:2], halves(error))


def solve_kernel(proj_ref, keys_ref, inv_ref, cross_ref, w_ref, u_ref, end_ref):
    count, size, _ = inv_ref.shape

    def given(n):
        part = slice(n * size, (n + 1) * size)
        return 2.0 * beside(keys_ref[part, :], proj_ref[part, 2 * DK :])

    for n in range(count // 2):
        first = wide3(halves(inv_ref[2 * n]), halves(given(2 * n)))
        later = given(2 * n + 1) - wide6(thirds(cross_ref[n]), thirds(first))
        second = wide3(halves(inv_ref[2 * n + 1]), halves(later))
        for at, found in ((2 * n, first), (2 * n + 1, second)):
            part = slice(at * size, (at + 1) * size)
            w_ref[part, :] = found[:, :DK]
            u_ref[part, :] = found[:, DK:]
    state = jnp.zeros((DK, DK), jnp.float32)
    for n in range(count // 2):
        part = slice(n * BLOCK, (n + 1) * BLOCK)
        fresh = u_ref[part, :]
        if n > 0:
            fresh = fresh - square3(halves(w_ref[part, :]), halves(state))
        state = state + dot3(keys_ref[part, :], fresh, ((0,), (0,)))
    end_ref[...] = state


def leave_kernel(start_ref, keys_ref, w_ref, u_ref, end_ref):
    state = start_ref[...]
    for n in range(keys_ref.shape[0] // BLOCK):
        part = pl.ds(n * BLOCK, BLOCK)
        fresh = u_ref[part, :] - dot3(w_ref[part, :], state)
        state = state + dot3(keys_ref[part, :], fresh, ((0,), (0,)))
    end_ref[...] = state


def output_kernel(at_ref, start_ref, q_ref, keys_ref, w_ref, u_ref, gain_ref, *outs):
    heads = len(outs)
    j = at_ref[0] % heads
    gain = gain_ref[j]
    row = lax.broadcasted_iota(jnp.int32, (BLOCK, BLOCK), 0)
    col = lax.broadcasted_iota(jnp.int32, (BLOCK, BLOCK), 1)
    state = start_ref[...]
    for n in range(keys_ref.shape[0] // BLOCK):
        part = pl.ds(n * BLOCK, BLOCK)
        raw = q_ref[part, :DK]
        queries = halves(raw * lax.rsqrt(jnp.sum(raw * raw, axis=-1, keepdims=True) + 1e-06))
        keys = halves(keys_ref[part, :])
        causal = jnp.where(row >= col, mul3(queries, keys, ((1,), (1,))), 0.0)
        entry = halves(state)
        fresh = halves(u_ref[part, :] - mul3(halves(w_ref[part, :]), entry))
        result = mul3(queries, entry) + mul3(halves(causal), fresh)
        state = state + mul3(keys, fresh, ((0,), (0,)))
        result = result * lax.rsqrt(jnp.mean(result * result, axis=-1, keepdims=True) + 1e-06) * gain
        for far in range(heads):

            @pl.when((j ^ far) == n)
            def _():
                outs[far][...] = result


def f32(*shape):
    return pltpu.VMEM(shape, jnp.float32)


def bf16(*shape):
    return pltpu.VMEM(shape, jnp.bfloat16)


def on_chip(n):
    return [pl.BlockSpec(memory_space=pltpu.VMEM)] * n


def kept(arrays):
    return [pltpu.with_memory_space_constraint(a, pltpu.VMEM) for a in arrays]


SCALARS = pl.BlockSpec(memory_space=pltpu.SMEM)
GROUPS = 4
ROOM = pltpu.CompilerParams(vmem_limit_bytes=16 * 2**20)


def chain_inverse(proj):
    rows = proj.shape[0]
    count, size = 2 * rows // BLOCK, BLOCK // 2
    return pl.pallas_call(
        inverse_kernel,
        in_specs=on_chip(1),
        out_specs=on_chip(3),
        out_shape=(f32(rows, DK), f32(count, size, size), f32(count // 2, size, size)),
        scratch_shapes=[pltpu.VMEM((count, size, size), jnp.float32)],
        cost_estimate=pl.CostEstimate(
            flops=40 * count * size**3, bytes_accessed=8 * rows * DK, transcendentals=rows
        ),
        compiler_params=ROOM,
        name="chain_inverse",
    )(*kept([proj]))


def chain_solve(proj, keys, inverse, cross):
    rows = proj.shape[0]
    return pl.pallas_call(
        solve_kernel,
        in_specs=on_chip(4),
        out_specs=on_chip(3),
        out_shape=(f32(rows, DK), f32(rows, DK), f32(DK, DK)),
        cost_estimate=pl.CostEstimate(flops=24 * rows * BLOCK * DK, bytes_accessed=20 * rows * DK, transcendentals=0),
        compiler_params=ROOM,
        name="chain_solve",
    )(*kept([proj, keys, inverse, cross]))


def chain_leave(start, keys, w, u):
    rows = keys.shape[0]
    return pl.pallas_call(
        leave_kernel,
        in_specs=on_chip(4),
        out_specs=on_chip(1)[0],
        out_shape=f32(DK, DK),
        cost_estimate=pl.CostEstimate(
            flops=3 * 4 * rows * DK * DK, bytes_accessed=12 * rows * DK, transcendentals=0
        ),
        compiler_params=ROOM,
        name="chain_leave",
    )(*kept([start, keys, w, u]))


def chain_output(start, proj, keys, w, u, gain, at, token_rows):
    rows = keys.shape[0]
    heads = rows // token_rows
    return pl.pallas_call(
        output_kernel,
        in_specs=[SCALARS] + on_chip(6),
        out_specs=on_chip(heads),
        out_shape=[f32(token_rows, DK)] * heads,
        cost_estimate=pl.CostEstimate(
            flops=3 * 2 * rows * DK * (3 * DK + 2 * BLOCK), bytes_accessed=20 * rows * DK, transcendentals=2 * rows
        ),
        compiler_params=ROOM,
        name="chain_output",
    )(at, *kept([start, proj, keys, w, u, gain]))


def columns_kernel(at_ref, w_ref, *outs):
    heads = len(outs)
    mine = at_ref[0] % heads
    for near in range(heads):
        for slot in range(heads):

            @pl.when((mine ^ near) == slot)
            def _():
                for part in range(w_ref.shape[0]):
                    outs[near][:, part * DK : (part + 1) * DK] = w_ref[part, :, slot * DK : (slot + 1) * DK]


def head_columns(at, w):
    parts, rows, width = w.shape
    return pl.pallas_call(
        columns_kernel,
        in_specs=[SCALARS] + on_chip(1),
        out_specs=on_chip(width // DK),
        out_shape=[f32(rows, parts * DK)] * (width // DK),
        compiler_params=ROOM,
        name="head_columns",
    )(at, w)


GROUPS = 4


def spread_kernel(at_ref, *refs):
    top_ref, rem_ref = refs[-2:]
    rows = refs[0].shape[0]
    for n, piece in enumerate(refs[:-2]):
        to = at_ref[1] ^ (n % GROUPS)
        part = pl.ds(n // GROUPS * rows, rows)
        top_ref[to, part, :], rem_ref[to, part, :] = halves(piece[...])


def spread(at, pieces):
    rows, feats = pieces[0].shape
    whole = (GROUPS, len(pieces) // GROUPS * rows, feats)
    return pl.pallas_call(
        spread_kernel,
        in_specs=[SCALARS] + on_chip(len(pieces)),
        out_specs=on_chip(2),
        out_shape=[bf16(*whole)] * 2,
        compiler_params=ROOM,
        name="spread",
    )(at, *kept(pieces))


def project_kernel(at_ref, *refs):
    tokens, weights, before = refs[:4], refs[4:6], refs[6:-5]
    out_ref, kv_top_ref, kv_rem_ref, q_both_ref, q_top_ref = refs[-5:]
    s, pair = at_ref[0], at_ref[2]
    j, z = s % GROUPS, s // 2
    rows = tokens[0].shape[1] // 2
    w_rows = weights[0].shape[0]
    for low in range(2):
        to = pl.ds(pl.multiple_of(((s & 1) ^ low) * w_rows, w_rows), w_rows)
        q_top, q_rem = halves(weights[low][:, :DK])
        q_top_ref[to, :] = q_top
        q_both_ref[to, :DK] = q_top
        q_both_ref[to, DK:] = q_rem
        kv_top_ref[to, :], kv_rem_ref[to, :] = halves(weights[low][:, DK:])
    dot = functools.partial(jnp.dot, preferred_element_type=jnp.float32)
    for at in range(4):
        to = pl.ds(pl.multiple_of((j ^ at) * rows, rows), rows)
        part = slice((at % 2) * rows, (at % 2 + 1) * rows)
        top, rem = tokens[at // 2 * 2][z ^ pair, part, :], tokens[at // 2 * 2 + 1][z ^ pair, part, :]
        kv = dot(top, kv_top_ref[...]) + (dot(top, kv_rem_ref[...]) + dot(rem, kv_top_ref[...]))
        both = dot(top, q_both_ref[...])
        q = both[:, :DK] + (both[:, DK:] + dot(rem, q_top_ref[...]))
        if before:
            kv = kv + before[0][to, DK:]
            q = q + before[0][to, :DK]
        out_ref[to, :DK] = q
        out_ref[to, DK:] = kv


def project(at, tokens, weights, before=None):
    _, two_rows, feats = tokens[0].shape
    _, width = weights[0].shape
    extra = [] if before is None else [before]
    rows = 2 * two_rows
    return pl.pallas_call(
        project_kernel,
        in_specs=[SCALARS] + on_chip(6 + len(extra)),
        out_specs=on_chip(1)[0],
        out_shape=f32(rows, width),
        scratch_shapes=[
            pltpu.VMEM((feats, width - DK), jnp.bfloat16),
            pltpu.VMEM((feats, width - DK), jnp.bfloat16),
            pltpu.VMEM((feats, 2 * DK), jnp.bfloat16),
            pltpu.VMEM((feats, DK), jnp.bfloat16),
        ],
        cost_estimate=pl.CostEstimate(
            flops=6 * rows * feats * width, bytes_accessed=4 * rows * feats, transcendentals=0
        ),
        compiler_params=ROOM,
        name="project",
    )(at, *kept([*tokens, *weights, *extra]))


def outward_kernel(heads, at_ref, *refs):
    pieces = refs[:heads]
    mine, sibling = refs[heads : heads + GROUPS], refs[heads + GROUPS : heads + 2 * GROUPS]
    outs = refs[heads + 2 * GROUPS : -2]
    top_ref, rem_ref = refs[-2:]
    s, h = at_ref[0], at_ref[1]
    j = s % heads
    for far in range(heads):
        top, rem = halves(pieces[far][...])
        for slot in range(heads):

            @pl.when((j ^ far) == slot)
            def _():
                top_ref[:, slot * DK : (slot + 1) * DK] = top
                rem_ref[:, slot * DK : (slot + 1) * DK] = rem

    left = (top_ref[...], rem_ref[...])
    odd = s % 2 == 1
    keep_ref, by_one_ref, by_two_ref, to_one_ref, to_two_ref = outs
    half = keep_ref.shape[0] // 2
    targets = (
        ((keep_ref, 0), (keep_ref, half)),
        ((to_one_ref, 0), (by_one_ref, 0)),
        ((by_two_ref, 0), (to_two_ref, 0)),
        ((to_one_ref, half), (to_two_ref, half)),
    )
    for at in range(GROUPS):
        there = (s // 2, (s // 2) ^ 1, 2 - s // heads, 3 - 3 * (s // heads))[at]
        one = mul3(left, halves(mine[at][...]))
        two = mul3(left, halves(sibling[at][...]))
        width = one.shape[1]
        first = jnp.where(odd, two, one)
        second = jnp.where(odd, one, two)
        for g in range(GROUPS):

            @pl.when((h ^ g) == there)
            def _():
                for n, (ref, to) in enumerate(targets[g]):
                    ref[to : to + half, :width] = first[n * half : (n + 1) * half]
                    ref[to : to + half, width:] = second[n * half : (n + 1) * half]


def outward(at, pieces, mine, sibling):
    heads = len(pieces)
    rows = pieces[0].shape[0]
    feats, width = mine[0].shape
    return pl.pallas_call(
        functools.partial(outward_kernel, heads),
        in_specs=[SCALARS] + on_chip(heads + 2 * GROUPS),
        out_specs=on_chip(5),
        compiler_params=ROOM,
        scratch_shapes=[pltpu.VMEM((rows, feats), jnp.bfloat16)] * 2,
        out_shape=[f32(count, 2 * width) for count in (rows, rows // 2, rows // 2, rows, rows)],
        cost_estimate=pl.CostEstimate(
            flops=12 * rows * feats * width * GROUPS, bytes_accessed=8 * GROUPS * feats * width, transcendentals=0
        ),
        name="outward",
    )(at, *kept([*pieces, *mine, *sibling]))


def by_xor(shard, axis, with_):
    size = lax.axis_size(axis)
    return lax.ppermute(shard, axis, [(i, i ^ with_) for i in range(size)])


def exchanged(inputs, w_project, w_output, norm_gain):
    rows, _ = inputs.shape
    heads = w_project.shape[2] // DK
    seq = lax.axis_size("seq")
    spans = seq // heads
    s = lax.axis_index("seq")
    h = lax.axis_index("head")
    first = jnp.arange(3, dtype=jnp.int32)
    at = (jnp.where(first == 0, s, 0) + jnp.where(first == 1, h, 0)).astype(jnp.int32)

    other = by_xor(inputs, "seq", 2)

    columns = head_columns(at, jnp.transpose(w_project, (1, 0, 2)))
    weights = [columns[far % heads] if far == 0 else by_xor(columns[far % heads], "seq", far) for far in range(seq)]

    blocks = [None] * heads
    for far, block in ((0, inputs), (2, other)):
        blocks[far] = [block] + [by_xor(block, "head", g) for g in range(1, GROUPS)]
        blocks[far + 1] = [by_xor(piece, "seq", 1) for piece in blocks[far]]
    tokens = []
    for n in range(0, heads, 2):
        tokens += spread(at, blocks[n] + blocks[n + 1])

    proj = None
    for pair in range(seq // 2):
        where = at + jnp.array([0, 0, pair], jnp.int32)
        proj = project(where, tokens, weights[2 * pair : 2 * pair + 2], proj)

    near_out = by_xor(w_output, "seq", 2)
    middle = [(i, i ^ 6) for i in range(seq) if i // 2 in (1, 2)]
    outer = [(i, i ^ 2) for i in range(seq) if i // 2 in (1, 2)]
    out_mine = [w_output, near_out]
    for block in (w_output, near_out):
        inner = lax.ppermute(block, "seq", middle)
        passed = lax.ppermute(inner, "seq", outer)
        out_mine.append(inner + passed)
    out_sibling = [by_xor(w, "seq", 1) for w in out_mine]

    keys, inverse, cross = chain_inverse(proj)
    w, u, leaving = chain_solve(proj, keys, inverse, cross)
    start = jnp.zeros((DK, DK), jnp.float32)
    for turn in range(spans - 1):
        if turn > 0:
            leaving = chain_leave(start, keys, w, u)
        start = from_behind(leaving, "seq", heads)
    normed = chain_output(start, proj, keys, w, u, norm_gain.reshape(heads, 1, DK), at, rows)

    pieces = [by_xor(piece, "seq", far) if far else piece for far, piece in enumerate(normed)]

    keep, by_one, by_two, to_one, to_two = outward(at, pieces, out_mine, out_sibling)
    half = rows // 2
    from_one = by_xor(to_one, "head", 1)
    from_two = by_xor(to_two, "head", 2)
    upper = by_xor(by_two + from_one[half:], "head", 2)
    lower = by_xor(by_one + from_two[half:], "head", 1)
    first = jnp.concatenate([from_one[:half], from_two[:half]], axis=0)
    return keep + first + jnp.concatenate([upper, lower], axis=0)


def power_of_two(n):
    return n > 0 and n & (n - 1) == 0


def solution(mesh):
    seq, groups = mesh.shape["seq"], mesh.shape["head"]

    def step(inputs, w_project, w_output, norm_gain):
        heads = w_project.shape[2] // DK
        fits = (
            power_of_two(seq)
            and power_of_two(groups)
            and power_of_two(heads)
            and 2 <= heads <= seq
            and groups == GROUPS
            and heads == GROUPS
            and seq == 2 * GROUPS
            and w_project.shape[0] * 2 == inputs.shape[1]
            and w_project.shape[0] % 8 == 0
            and inputs.shape[0] == BLOCK
        )
        if not fits:
            return general(inputs, w_project, w_output, norm_gain)
        return exchanged(inputs, w_project, w_output, norm_gain)

    return jax.shard_map(
        step,
        mesh=mesh,
        in_specs=(P("seq", "head"), P("seq", None, "head"), P("head", "seq"), P("head")),
        out_specs=P("seq", "head"),
        check_vma=False,
    )
```
